128 devices in a mesh: dp: 8 (over z_hi, x), seq: 16 (over z_lo, y, core).
Axes of the slice: x: 4, y: 4, z: 4 (z_hi: 2, z_lo: 2; z = z_hi * 2 + z_lo), core: 2. Of those that a mesh axis runs over, the one named last changes fastest.
Arguments:
- stream: bfloat16 [8, 512, 1536], P('dp', 'seq'), may hold values from -6 to 6
- queries: bfloat16 [8, 512, 1536], P('dp', 'seq'), may hold values from -30 to 30
- new_keys: bfloat16 [8, 512, 1536], P('dp', 'seq'), may hold values from -6.5 to 6.5
- new_values: bfloat16 [8, 512, 1536], P('dp', 'seq'), may hold values from -6 to 6
- cache_keys: bfloat16 [8, 1536, 1536], P('dp', 'seq'), may hold values from -6.375 to 6.375
- cache_values: bfloat16 [8, 1536, 1536], P('dp', 'seq'), may hold values from -6 to 6
- cache_frames: int32 [8, 1536], P('dp', 'seq'), may hold values from 0 to 20, as said below
- group_index: int32 [8], P('dp'), may hold values from 4 to 7, as said below
- timestep: int32 [8], P('dp'), may hold values from 0 to 3
- gate_table: float32 [4, 1536], replicated, may hold values from 0.1 to 1.9
- attn_out_weight: bfloat16 [1536, 1536], replicated, may hold values from -0.15625 to 0.15625
- critic_in: bfloat16 [131072, 1536], P(('dp', 'seq')), may hold values from -24 to 24
- critic_cot: bfloat16 [131072, 1536], P(('dp', 'seq')), may hold values from -6 to 6
- critic_weight: bfloat16 [1536, 1536], P(('dp', 'seq')), may hold values from -0.15625 to 0.15625
Outputs:
- stream_out: bfloat16 [8, 512, 1536], P('dp', 'seq')
- critic_grad_in: bfloat16 [131072, 1536], P(('dp', 'seq'))
- critic_grad_weight: float32 [1536, 1536], P(('dp', 'seq'))
The draws below stay inside these ranges and needn't reach their ends.
Inputs may be any that keep to these rules, and one draw needn't show every extreme that they name: `group_index`: index of the frame group; both ends are reached in every draw. `cache_frames`: sample b's cache holds the 12 frames 3 * group_index[b] - 12 to 3 * group_index[b] - 1, each in one contiguous run of slots, runs of equal length up to one slot, in a rotated order.
All inputs are finite; a program needn't handle non-finite values.
Results may differ from the reference program's by a relative error of at most 0.0045.
Values may be sent and summed in bfloat16 or wider, within the bound.
No kernel may reach another device: no remote copies, remote signals or barrier semaphores. Data moves between devices by JAX's collectives and lax.ppermute only.
A program may use at most 128 MiB of HBM per device.

```python
import jax
import jax.numpy as jnp
from jax import lax

D = 1536
HEADS = 12
HEAD = 128
STEPS = 4
FRAMES_GROUP = 3
WINDOW_FRAMES = 9
BATCH = 8
GROUP = 512
CACHE = 1536
CRIT_ROWS = 131072


def drawn_pair(key):
    base = jax.random.fold_in(key, 4711)
    key_q, key_k = jax.random.split(base, 2)
    query_draw = jnp.clip(1.6 * jax.random.normal(key_q, (BATCH, GROUP, D), jnp.float32), -6.4, 6.4)
    key_draw = jnp.clip(1.6 * jax.random.normal(key_k, (BATCH, GROUP, D), jnp.float32), -6.4, 6.4)
    return (query_draw, key_draw)


def draw_queries(key, part):
    return drawn_pair(key)[0].astype(jnp.bfloat16)


def draw_new_keys(key, part):
    return drawn_pair(key)[1].astype(jnp.bfloat16)


def frame_layout(key):
    base = jax.random.fold_in(key, 9173)
    key_group, key_turn = jax.random.split(base, 2)
    cycle = FRAMES_GROUP + WINDOW_FRAMES
    group = jax.random.randint(key_group, (BATCH,), 4, 8, dtype=jnp.int32)
    group = group.at[0].set(7).at[BATCH - 1].set(4)
    turn = jax.random.randint(key_turn, (BATCH, 1), 0, cycle, dtype=jnp.int32)
    block = jnp.arange(CACHE, dtype=jnp.int32) * cycle // CACHE
    frames = FRAMES_GROUP * group[:, None] - cycle + (block[None, :] + turn) % cycle
    return (group, frames.astype(jnp.int32))


def draw_group_index(key, part):
    return frame_layout(key)[0]


def draw_cache_frames(key, part):
    return frame_layout(key)[1]


def plant(drawn, own_key, low, top_value):
    longest = drawn.shape.index(max(drawn.shape))
    spots = []
    for shift in (0, 1):
        where = [jax.random.randint(jax.random.fold_in(own_key, axis), (), 0, length) for axis, length in enumerate(drawn.shape)]
        where[longest] = (where[longest] + shift) % drawn.shape[longest]
        spots.append(tuple(where))
    return drawn.at[spots[0]].set(low).at[spots[1]].set(top_value)


def strengthened(entries, stream_key, source, target, parts, factor):
    def block_of(axis_at):
        return (jnp.arange(entries.shape[axis_at]) // (entries.shape[axis_at] // parts)).reshape((-1,) + (1,) * (entries.ndim - 1 - axis_at))

    one_side = jax.random.permutation(stream_key, parts)[block_of(target)]
    other_side = (block_of(target) + parts // 2) % parts
    return jnp.where((block_of(source) == one_side) | (block_of(source) == other_side), factor * entries, entries)


def shard_levels(key, shape, cuts, least, largest):
    def one(position, shards_of):
        heights = jax.random.uniform(jax.random.fold_in(jax.random.fold_in(key, 6), position), (shards_of,), jnp.float32, least / len(cuts), largest / len(cuts))
        return jnp.repeat(jnp.exp(heights), shape[position] // shards_of).reshape((-1,) + (1,) * (len(shape) - position - 1))

    loudness = one(*cuts[0])
    for cut in cuts[1:]:
        loudness = loudness * one(*cut)
    return loudness


def noise(key, shape, spread, limit, cuts=(), held_as=jnp.bfloat16):
    factor_of = shard_levels(key, shape, cuts, -0.22, 0.18) if cuts else 1.0
    values = jax.random.normal(key, shape, jnp.float32) * spread * factor_of
    return jnp.minimum(jnp.maximum(values, -limit), limit).astype(held_as)


def noise_with(key, shape, scale, bound, cuts, heavy, kind=jnp.bfloat16):
    array = scale * jax.random.normal(key, shape, jnp.float32)
    if cuts:
        array = array * shard_levels(key, shape, cuts, -0.22, 0.18)
    return jnp.clip(strengthened(array, jax.random.fold_in(key, 3), *heavy), -bound, bound).astype(kind)


def setup_inputs(seed: int = 0) -> dict:
    key_list = jax.random.split(jax.random.key(seed), 15)
    stream = noise(key_list[0], (BATCH, GROUP, D), 1.0, 6.0, ((0, 8), (1, 16)))
    queries = draw_queries(jax.random.fold_in(key_list[14], 71), 0)
    new_keys = draw_new_keys(jax.random.fold_in(key_list[14], 71), 0)
    new_values = noise(key_list[3], (BATCH, GROUP, D), 1.0, 6.0, ((0, 8), (1, 16)))
    cache_keys = noise(key_list[4], (BATCH, CACHE, D), 1.6, 6.375, ((0, 8), (1, 16)))
    cache_values = noise(key_list[5], (BATCH, CACHE, D), 1.0, 6.0, ((0, 8), (1, 16)))
    cache_frames = draw_cache_frames(jax.random.fold_in(key_list[14], 71), 0)
    group_index = draw_group_index(jax.random.fold_in(key_list[14], 71), 0)
    timestep = plant(jax.random.randint(key_list[8], (BATCH,), 0, STEPS), jax.random.fold_in(key_list[8], 1), 0, STEPS - 1).astype(jnp.int32)
    gate_table = jnp.clip(1.0 + 0.18 * jax.random.normal(key_list[9], (STEPS, D), jnp.float32), 0.1, 1.9)
    attn_out_weight = noise(key_list[10], (D, D), D ** -0.5, 0.15625)
    critic_in = noise_with(key_list[11], (CRIT_ROWS, D), 1.0, 24.0, ((0, 128),), (0, 1, 128, 5.5))
    critic_cot = noise(key_list[12], (CRIT_ROWS, D), 1.0, 6.0, ((0, 128),))
    critic_weight = noise(key_list[13], (D, D), D ** -0.5, 0.15625, ((0, 128),))
    return {"stream": stream, "queries": queries, "new_keys": new_keys, "new_values": new_values, "cache_keys": cache_keys, "cache_values": cache_values, "cache_frames": cache_frames, "group_index": group_index, "timestep": timestep, "gate_table": gate_table, "attn_out_weight": attn_out_weight, "critic_in": critic_in, "critic_cot": critic_cot, "critic_weight": critic_weight}


def attend_sample(packed):
    query_block, key_new, value_new, key_cache, value_cache, frames, group = packed
    keys = jnp.concatenate([key_cache, key_new], axis=0)
    values = jnp.concatenate([value_cache, value_new], axis=0)
    first = FRAMES_GROUP * group
    live_cache = (frames < first) & (frames >= first - WINDOW_FRAMES)
    live = jnp.concatenate([live_cache, jnp.ones((GROUP,), dtype=bool)])
    query_heads = query_block.reshape(GROUP, HEADS, HEAD).transpose(1, 0, 2)
    key_heads = keys.reshape(GROUP + CACHE, HEADS, HEAD).transpose(1, 0, 2)
    value_heads = values.reshape(GROUP + CACHE, HEADS, HEAD).transpose(1, 0, 2)

    def one_head(triple):
        q_head, k_head, v_head = triple
        scores = jnp.dot(q_head, k_head.T, preferred_element_type=jnp.float32) * (HEAD ** -0.5)
        scores = jnp.where(live[None, :], scores, -1e30)
        top = jnp.max(scores, axis=1, keepdims=True)
        weights = jnp.where(live[None, :], jnp.exp(scores - top), 0.0)
        totals = jnp.sum(weights, axis=1, keepdims=True)
        summed = jnp.dot(weights.astype(jnp.bfloat16), v_head, preferred_element_type=jnp.float32)
        return summed / totals

    mixed = lax.map(one_head, (query_heads, key_heads, value_heads))
    return mixed.transpose(1, 0, 2).reshape(GROUP, D).astype(jnp.bfloat16)


def reference(stream, queries, new_keys, new_values, cache_keys, cache_values, cache_frames, group_index, timestep, gate_table, attn_out_weight, critic_in, critic_cot, critic_weight):
    mixed = lax.map(attend_sample, (queries, new_keys, new_values, cache_keys, cache_values, cache_frames, group_index))
    projected = jnp.dot(mixed.reshape(BATCH * GROUP, D), attn_out_weight, preferred_element_type=jnp.float32).reshape(BATCH, GROUP, D)
    onehot = (timestep[:, None] == jnp.arange(STEPS, dtype=jnp.int32)[None, :]).astype(jnp.float32)
    gate = jnp.dot(onehot, gate_table, precision=lax.Precision.HIGHEST)
    stream_out = (stream.astype(jnp.float32) + gate[:, None, :] * projected).astype(jnp.bfloat16)
    grad_in = jnp.dot(critic_cot, critic_weight.T, preferred_element_type=jnp.float32).astype(jnp.bfloat16)
    grad_weight = jnp.dot(critic_in.T, critic_cot, preferred_element_type=jnp.float32) * (float(CRIT_ROWS) ** -0.5)
    return (stream_out, grad_in, grad_weight)
```

```python
import jax
import jax.numpy as jnp
from jax import lax
from jax.experimental import pallas as pl
from jax.experimental.pallas import tpu as pltpu
from jax.sharding import Mesh
from jax.sharding import PartitionSpec as P

HEADS = 12
HEAD = 128
FRAMES_GROUP = 3
WINDOW_FRAMES = 9
BF = jnp.bfloat16
F32 = jnp.float32


SWAP = [(0, 1), (1, 0)]


def turn(k):
    return [(i, (i + k) % 4) for i in range(4)]


def pick(array, index, dim):
    return lax.dynamic_index_in_dim(array, index, dim, keepdims=False)


def attend(q, k, v, live):
    rows = 128

    def kernel(q_ref, k_ref, v_ref, live_ref, out_ref):
        lane = lax.broadcasted_iota(jnp.int32, (rows, HEAD), 1)
        alive = live_ref[0:1, :] > 0.5
        for r in range(q_ref.shape[0] // rows):
            stats = jnp.zeros((rows, HEAD), F32)
            for h in range(3):
                cols = slice(h * HEAD, (h + 1) * HEAD)
                s = lax.dot_general(
                    q_ref[r * rows : (r + 1) * rows, cols],
                    k_ref[:, cols],
                    (((1,), (1,)), ((), ())),
                    preferred_element_type=F32,
                ) * (HEAD ** (-0.5))
                s = jnp.where(alive, s, -1e30)
                top = jnp.max(s, axis=1, keepdims=True).astype(BF).astype(F32)
                w = jnp.where(alive, jnp.exp(s - top), 0.0)
                total = jnp.sum(w, axis=1, keepdims=True)
                o = jnp.dot(w.astype(BF), v_ref[:, cols], preferred_element_type=F32)
                out_ref[r * rows : (r + 1) * rows, cols] = o.astype(BF)
                high = total.astype(BF).astype(F32)
                stats = jnp.where(lane == h, top, stats)
                stats = jnp.where(lane == 4 + h, high, stats)
                stats = jnp.where(lane == 8 + h, total - high, stats)
            out_ref[r * rows : (r + 1) * rows, 3 * HEAD :] = stats.astype(BF)

    return pl.pallas_call(
        kernel,
        out_shape=jax.ShapeDtypeStruct((q.shape[0], 4 * HEAD), BF),
        name="attend",
    )(q, k, v, live)


def merged(parts):
    parts = [p.astype(F32) for p in parts]
    base = 3 * HEAD
    tops = [p[:, base : base + 3] for p in parts]
    totals = [p[:, base + 4 : base + 7] + p[:, base + 8 : base + 11] for p in parts]
    top = tops[0]
    for t in tops[1:]:
        top = jnp.maximum(top, t)
    scales = [jnp.exp(t - top) for t in tops]
    total = sum(s * t for s, t in zip(scales, totals))
    rows = parts[0].shape[0]
    summed = sum(
        p[:, :base].reshape(rows, 3, HEAD) * s[:, :, None] for p, s in zip(parts, scales)
    )
    return (summed / total[:, :, None]).reshape(rows, base).astype(BF)


def ordered_rows(own, other, place):
    pieces = own + other
    width = own[0].shape[-1]
    steps = (0, 3, 1, 2)

    def kernel(place_ref, *refs):
        ins, (out_ref, buf, sem) = refs[: len(pieces)], refs[len(pieces) :]
        zl, y, c = place_ref[0], place_ref[1], place_ref[2]
        copies = []
        for n in range(len(pieces)):
            core = c if n < 4 else 1 - c
            yy = (y + steps[n % 4]) % 4
            for far in range(2):
                zz = zl if far == 0 else 1 - zl
                copy = pltpu.make_async_copy(
                    ins[n].at[far], buf.at[zz * 8 + yy * 2 + core], sem.at[n * 2 + far]
                )
                copy.start()
                copies.append(copy)
        for copy in copies:
            copy.wait()
        for d in range(8):
            for t in range(4):
                rows = [buf[t * 4 + k, 12 * d : 12 * d + 12, :] for k in range(4)]
                at = d * 192 + t * 48
                out_ref[at : at + 48, :] = jnp.concatenate(rows, axis=0)

    return pl.pallas_call(
        kernel,
        out_shape=jax.ShapeDtypeStruct((1536, width), BF),
        in_specs=[pl.BlockSpec(memory_space=pltpu.SMEM)]
        + [pl.BlockSpec(memory_space=pl.ANY)] * len(pieces),
        scratch_shapes=[
            pltpu.VMEM((16, 96, width), BF),
            pltpu.SemaphoreType.DMA((16,)),
        ],
        name="ordered_rows",
    )(place, *pieces)


def whole_weight(weight, zh, x, zl, y, c):
    ring = [weight] + [lax.ppermute(weight, "x", turn(-k)) for k in (1, 2, 3)]
    ring = jnp.stack(ring + ring)
    on_x = lax.dynamic_slice_in_dim(ring, (4 - x) % 4, 4, 0).reshape(48, -1)
    far = lax.ppermute(on_x, "zh", SWAP)
    here = jnp.where(zh == 0, jnp.concatenate([on_x, far]), jnp.concatenate([far, on_x]))
    near = jnp.stack([here, lax.ppermute(here, "zl", SWAP)])
    before = lax.ppermute(near, "y", turn(1))
    after = lax.ppermute(near, "y", turn(-1))
    cross = jnp.stack(
        [lax.ppermute(after[0], "y", turn(-1)), lax.ppermute(before[1], "y", turn(1))]
    )
    own = [near, before, after, cross]
    other = [lax.ppermute(p, "c", SWAP) for p in own]
    return ordered_rows(own, other, jnp.stack([zl, y, c]).astype(jnp.int32))


def weight_gradient(critic_in, critic_cot, zh, x, zl, y, c, factor):
    width = critic_cot.shape[1]
    half = width // 2

    def product(cols):
        return (
            lax.dot_general(
                critic_in, cols, (((0,), (0,)), ((), ())), preferred_element_type=F32
            )
            * factor
        )

    theirs = product(lax.dynamic_slice_in_dim(critic_cot, (1 - c) * half, half, 1)).astype(BF)
    got = lax.ppermute(theirs, "c", SWAP)
    mine = product(lax.dynamic_slice_in_dim(critic_cot, c * half, half, 1)) + got.astype(F32)
    blocks = mine.reshape(2, 4, 192, half)

    def over_x(part, first, second, first_perm, second_perm):
        there = first
        send = jnp.stack([pick(part, there, 1), pick(part, second(there), 1)]).astype(BF)
        got = lax.ppermute(send, "x", first_perm).astype(F32)
        onward = (pick(part, second(x), 1) + got[1]).astype(BF)
        last = lax.ppermute(onward, "x", second_perm).astype(F32)
        return pick(part, x, 1) + got[0] + last

    near = [(0, 1), (1, 0), (2, 3), (3, 2)]
    wrap = [(0, 3), (3, 0), (1, 2), (2, 1)]
    left = over_x(blocks[..., : half // 2], x ^ 1, lambda i: 3 - i, near, wrap)
    right = over_x(blocks[..., half // 2 :], 3 - x, lambda i: i ^ 1, wrap, near)
    rows = jnp.concatenate([left, right], axis=-1).reshape(2, 2, 4, 24, half)

    total = pick(rows, y, 2)
    for k in (1, 2, 3):
        send = pick(rows, (y + k) % 4, 2).astype(BF)
        total = total + lax.ppermute(send, "y", turn(k)).astype(F32)
    total = pick(total, zh, 0) + lax.ppermute(pick(total, 1 - zh, 0), "zh", SWAP)
    total = pick(total, zl, 0) + lax.ppermute(pick(total, 1 - zl, 0), "zl", SWAP)
    total = total.reshape(2, 12, half)
    far = lax.ppermute(pick(total, 1 - c, 0), "c", SWAP)
    own = pick(total, c, 0)
    return jnp.where(
        c == 0, jnp.concatenate([own, far], axis=1), jnp.concatenate([far, own], axis=1)
    )


def local(
    stream,
    queries,
    new_keys,
    new_values,
    cache_keys,
    cache_values,
    cache_frames,
    group_index,
    timestep,
    gate_table,
    attn_out_weight,
    critic_in,
    critic_cot,
    critic_weight,
):
    zh, x, zl, y, c = (lax.axis_index(a) for a in ("zh", "x", "zl", "y", "c"))
    width = queries.shape[2]
    half, quarter = width // 2, width // 4
    first_frame = FRAMES_GROUP * group_index[0]
    frames = cache_frames[0]
    live_cache = (frames < first_frame) & (frames >= first_frame - WINDOW_FRAMES)
    live = jnp.concatenate([live_cache.astype(BF), jnp.ones((32,), BF)])
    live_row = jnp.tile(jnp.concatenate([live, jnp.zeros((quarter - 128,), BF)]), 4)
    live_rows = jnp.broadcast_to(live_row[None, :], (16, width))

    pack = jnp.concatenate(
        [cache_keys[0], new_keys[0], cache_values[0], new_values[0], queries[0], live_rows], axis=0
    )
    mine = lax.dynamic_slice_in_dim(pack, c * half, half, 1)
    theirs = lax.dynamic_slice_in_dim(pack, (1 - c) * half, half, 1)
    both = jnp.stack([mine, lax.ppermute(theirs, "c", SWAP)])
    keep = lax.dynamic_slice_in_dim(both, zl * quarter, quarter, 2)
    send = lax.dynamic_slice_in_dim(both, (1 - zl) * quarter, quarter, 2)
    sets = jnp.concatenate([keep, lax.ppermute(send, "zl", SWAP)])
    keys = sets[:, :128].reshape(512, quarter)
    values = sets[:, 128:256].reshape(512, quarter)
    own_queries = sets[:, 256:288].reshape(128, quarter)
    alive = jnp.broadcast_to(sets[:, 288, :128].reshape(1, 512).astype(F32), (8, 512))
    all_queries = jnp.concatenate(
        [own_queries] + [lax.ppermute(own_queries, "y", turn(k)) for k in (1, 2, 3)]
    )
    partial = attend(all_queries, keys, values, alive).reshape(4, 128, 4 * HEAD)
    parts = [partial[0]] + [lax.ppermute(partial[k], "y", turn(-k)) for k in (1, 2, 3)]
    mixed = merged(parts)
    got = lax.ppermute(mixed[64:], "zl", SWAP)
    own = mixed[:64]
    wide = jnp.where(
        zl == 0, jnp.concatenate([own, got], axis=1), jnp.concatenate([got, own], axis=1)
    )
    got = lax.ppermute(wide[32:], "c", SWAP)
    own = wide[:32]
    mixed = jnp.where(
        c == 0, jnp.concatenate([own, got], axis=1), jnp.concatenate([got, own], axis=1)
    )
    projected = jnp.dot(mixed, attn_out_weight, preferred_element_type=F32)
    onehot = (
        timestep[:, None] == jnp.arange(gate_table.shape[0], dtype=jnp.int32)[None, :]
    ).astype(F32)
    gate = jnp.dot(onehot, gate_table, precision=lax.Precision.HIGHEST)
    stream_out = (stream[0].astype(F32) + gate * projected).astype(BF)[None]

    weight = whole_weight(critic_weight, zh, x, zl, y, c)
    grad_in = lax.dot_general(
        critic_cot, weight, (((1,), (1,)), ((), ())), preferred_element_type=F32
    ).astype(BF)
    factor = float(critic_in.shape[0] * 128) ** (-0.5)
    grad_weight = weight_gradient(critic_in, critic_cot, zh, x, zl, y, c, factor)
    return (stream_out, grad_in, grad_weight)


def solution(mesh):
    cut = Mesh(mesh.devices.reshape(2, 4, 2, 4, 2), ("zh", "x", "zl", "y", "c"))
    dp, seq = ("zh", "x"), ("zl", "y", "c")
    whole = dp + seq
    return jax.shard_map(
        local,
        mesh=cut,
        in_specs=(
            P(dp, seq, None),
            P(dp, seq, None),
            P(dp, seq, None),
            P(dp, seq, None),
            P(dp, seq, None),
            P(dp, seq, None),
            P(dp, seq),
            P(dp),
            P(dp),
            P(),
            P(),
            P(whole, None),
            P(whole, None),
            P(whole, None),
        ),
        out_specs=(P(dp, seq, None), P(whole, None), P(whole, None)),
        check_vma=False,
    )
```

```python
import jax
import jax.numpy as jnp
from jax import lax
from jax.experimental import pallas as pl
from jax.experimental.pallas import tpu as pltpu
from jax.sharding import Mesh
from jax.sharding import PartitionSpec as P

HEADS = 12
HEAD = 128
FRAMES_GROUP = 3
WINDOW_FRAMES = 9
BF = jnp.bfloat16
F32 = jnp.float32


SWAP = [(0, 1), (1, 0)]


def turn(k):
    return [(i, (i + k) % 4) for i in range(4)]


def pick(array, index, dim):
    return lax.dynamic_index_in_dim(array, index, dim, keepdims=False)


def any_spec():
    return pl.BlockSpec(memory_space=pl.ANY)


def scalars():
    return pl.BlockSpec(memory_space=pltpu.SMEM)


def packed(place, group_index, frames, arrays):
    width = arrays[0].shape[1]
    quarter = width // 4
    starts, total = [], 0
    for a in arrays:
        starts.append(total)
        total += a.shape[0]

    def kernel(place_ref, group_ref, frames_ref, *refs):
        ins, outs, live_ref = refs[:5], refs[5:9], refs[9]
        first = FRAMES_GROUP * group_ref[0]
        f = frames_ref[...]
        live_ref[...] = jnp.zeros_like(live_ref)
        live_ref[:, 0:128] = jnp.ones((16, 128), F32)
        alive = (f < first) & (f >= first - WINDOW_FRAMES)
        live_ref[:, 0:96] = jnp.broadcast_to(alive.astype(F32), (16, 96))
        spot = place_ref[2] * 2 + place_ref[0]
        for here in range(4):

            @pl.when(spot == here)
            def _():
                for n, q in enumerate((here, here ^ 1, here ^ 2, here ^ 3)):
                    for a, at in zip(ins, starts):
                        outs[n][at : at + a.shape[0], :] = a[:, q * quarter : (q + 1) * quarter]

        for out in outs:
            out[total : total + 16, :] = live_ref[...].astype(BF)

    return pl.pallas_call(
        kernel,
        out_shape=[jax.ShapeDtypeStruct((total + 16, quarter), BF)] * 4,
        in_specs=[scalars(), scalars()] + [pl.BlockSpec()] * 6,
        scratch_shapes=[pltpu.VMEM((16, quarter), F32)],
        name="packed",
    )(place, group_index, frames, *arrays)


def attend(sets, queries):
    quarter = 3 * HEAD

    def kernel(*refs):
        set_refs, query_refs, outs = refs[:4], refs[4:8], refs[8:]
        rows = 128
        lane = lax.broadcasted_iota(jnp.int32, (rows, HEAD), 1)
        alive = jnp.concatenate([r[288:304, 0:128] for r in set_refs], axis=1)
        alive = alive.astype(F32)[0:1, :] > 0.5
        stats = [jnp.zeros((rows, HEAD), F32) for _ in range(4)]
        for h in range(3):
            cols = slice(h * HEAD, (h + 1) * HEAD)
            k = jnp.concatenate([r[0:128, cols] for r in set_refs], axis=0)
            v = jnp.concatenate([r[128:256, cols] for r in set_refs], axis=0)
            for r in range(4):
                s = lax.dot_general(
                    query_refs[r][:, cols], k, (((1,), (1,)), ((), ())), preferred_element_type=F32
                ) * (HEAD ** (-0.5))
                s = jnp.where(alive, s, -1e30)
                top = jnp.max(s, axis=1, keepdims=True).astype(BF).astype(F32)
                w = jnp.where(alive, jnp.exp(s - top), 0.0)
                total = jnp.sum(w, axis=1, keepdims=True)
                o = jnp.dot(w.astype(BF), v, preferred_element_type=F32)
                outs[r][:, cols] = o.astype(BF)
                high = total.astype(BF).astype(F32)
                stats[r] = jnp.where(lane == h, top, stats[r])
                stats[r] = jnp.where(lane == 4 + h, high, stats[r])
                stats[r] = jnp.where(lane == 8 + h, total - high, stats[r])
        for r in range(4):
            outs[r][:, quarter:] = stats[r].astype(BF)

    return pl.pallas_call(
        kernel,
        out_shape=[jax.ShapeDtypeStruct((128, 4 * HEAD), BF)] * 4,
        name="attend",
    )(*sets, *queries)


def merged(parts):
    def kernel(*refs):
        ins, outs = refs[:4], refs[4:]
        base = 3 * HEAD
        stats = [r[:, base:].astype(F32) for r in ins]
        for h in range(3):
            tops = [s[:, h : h + 1] for s in stats]
            totals = [s[:, 4 + h : 5 + h] + s[:, 8 + h : 9 + h] for s in stats]
            top = jnp.maximum(jnp.maximum(tops[0], tops[1]), jnp.maximum(tops[2], tops[3]))
            scales = [jnp.exp(t - top) for t in tops]
            total = sum(a * b for a, b in zip(scales, totals))
            cols = slice(h * HEAD, (h + 1) * HEAD)
            summed = sum(r[:, cols].astype(F32) * a for r, a in zip(ins, scales))
            mixed = (summed / total).astype(BF)
            for n in range(4):
                outs[n][:, cols] = mixed[32 * n : 32 * n + 32]

    return pl.pallas_call(
        kernel,
        out_shape=[jax.ShapeDtypeStruct((32, 3 * HEAD), BF)] * 4,
        name="merged",
    )(*parts)


def streamed(place, timestep, stream, gate_table, mixed, weight):
    width = weight.shape[1]
    quarter = width // 4

    def kernel(place_ref, step_ref, stream_ref, gate_ref, a_ref, b_ref, c_ref, d_ref, w_ref, out_ref):
        spot = place_ref[2] * 2 + place_ref[0]
        for here in range(4):

            @pl.when(spot == here)
            def _():
                total = jnp.zeros(out_ref.shape, F32)
                for ref, q in zip((a_ref, b_ref, c_ref, d_ref), (here, here ^ 2, here ^ 1, here ^ 3)):
                    total = total + jnp.dot(
                        ref[...], w_ref[q * quarter : (q + 1) * quarter, :], preferred_element_type=F32
                    )
                gate = gate_ref[pl.ds(step_ref[0], 1), :]
                out_ref[...] = (stream_ref[...].astype(F32) + gate * total).astype(BF)

    return pl.pallas_call(
        kernel,
        out_shape=jax.ShapeDtypeStruct(stream.shape, BF),
        in_specs=[scalars(), scalars()] + [pl.BlockSpec()] * 7,
        name="streamed",
    )(place, timestep, stream, gate_table, *mixed, weight)


def grad_of_input(place, cot, pieces):
    rows, width = cot.shape
    block = 256
    keys = [k for k, _ in pieces]
    count = len(pieces)

    def kernel(place_ref, cot_ref, *refs):
        ins, (out_ref, buf, weight, sem) = refs[:count], refs[count:]
        zl, y, c, zh, x = (place_ref[n] for n in range(5))

        @pl.when(pl.program_id(0) == 0)
        def _():
            copies = []
            for n, (far, step, other) in enumerate(keys):
                zz = 1 - zl if far else zl
                yy = (y + step) % 4
                cc = 1 - c if other else c
                copies.append(
                    pltpu.make_async_copy(ins[n], buf.at[zz * 8 + yy * 2 + cc], sem.at[n])
                )
                copies[-1].start()
            for copy in copies:
                copy.wait()
            for far in range(2):
                for step in range(4):
                    zz = 1 - zh if far else zh
                    xx = (x + 4 - step) % 4
                    at = 12 * (4 * far + step)
                    for t in range(4):
                        part = [buf[t * 4 + k, at : at + 12, :] for k in range(4)]
                        base = pl.multiple_of(zz * 768 + xx * 192 + t * 48, 16)
                        weight[pl.ds(base, 48), :] = jnp.concatenate(part, axis=0)

        out_ref[...] = lax.dot_general(
            cot_ref[...], weight[...], (((1,), (1,)), ((), ())), preferred_element_type=F32
        ).astype(BF)

    return pl.pallas_call(
        kernel,
        grid=(rows // block,),
        out_shape=jax.ShapeDtypeStruct((rows, width), BF),
        in_specs=[scalars(), pl.BlockSpec((block, width), lambda i: (i, 0))] + [any_spec()] * count,
        out_specs=pl.BlockSpec((block, width), lambda i: (i, 0)),
        scratch_shapes=[
            pltpu.VMEM((16, 96, width), BF),
            pltpu.VMEM((width, width), BF),
            pltpu.SemaphoreType.DMA((count,)),
        ],
        compiler_params=pltpu.CompilerParams(dimension_semantics=("arbitrary",)),
        name="grad_of_input",
    )(place, cot, *[p for _, p in pieces])


def weight_pieces(weight):
    on_x = jnp.concatenate([weight] + [lax.ppermute(weight, "x", turn(k)) for k in (1, 2, 3)])
    near = jnp.concatenate([on_x, lax.ppermute(on_x, "zh", SWAP)])
    far = lax.ppermute(near, "zl", SWAP)
    pieces = {(0, 0): near, (1, 0): far}
    for f in range(2):
        pieces[f, 3] = lax.ppermute(pieces[f, 0], "y", turn(1))
        pieces[f, 1] = lax.ppermute(pieces[f, 0], "y", turn(-1))
    pieces[0, 2] = lax.ppermute(pieces[0, 1], "y", turn(-1))
    pieces[1, 2] = lax.ppermute(pieces[1, 3], "y", turn(1))
    out = [((f, step, 0), p) for (f, step), p in pieces.items()]
    out += [((f, step, 1), lax.ppermute(p, "c", SWAP)) for (f, step), p in pieces.items()]
    return out


def weight_gradient(critic_in, critic_cot, zh, x, zl, y, c, factor):
    width = critic_cot.shape[1]
    half = width // 2

    def product(cols):
        return (
            lax.dot_general(
                cols, critic_cot, (((0,), (0,)), ((), ())), preferred_element_type=F32
            )
            * factor
        )

    theirs = product(lax.dynamic_slice_in_dim(critic_in, (1 - c) * half, half, 1)).astype(BF)
    got = lax.ppermute(theirs, "c", SWAP)
    mine = product(lax.dynamic_slice_in_dim(critic_in, c * half, half, 1)) + got.astype(F32)
    blocks = mine.reshape(4, 192, width)

    def over_x(part, first, second, first_perm, second_perm):
        send = jnp.stack([pick(part, first, 0), pick(part, second(first), 0)]).astype(BF)
        got = lax.ppermute(send, "x", first_perm).astype(F32)
        onward = (pick(part, second(x), 0) + got[1]).astype(BF)
        last = lax.ppermute(onward, "x", second_perm).astype(F32)
        return pick(part, x, 0) + got[0] + last, send

    near = [(0, 1), (1, 0), (2, 3), (3, 2)]
    wrap = [(0, 3), (3, 0), (1, 2), (2, 1)]
    left, sent = over_x(blocks[..., :half], x ^ 1, lambda i: 3 - i, near, wrap)
    right, _ = over_x(blocks[..., half:], 3 - x, lambda i: i ^ 1, wrap, near)
    rows = jnp.concatenate([left, right], axis=-1).reshape(2, 4, 24, width)

    total = pick(rows, y, 1)
    for k in (1, 2, 3):
        send = pick(rows, (y + k) % 4, 1).astype(BF)
        total = total + lax.ppermute(send, "y", turn(k)).astype(F32)
    total = pick(total, zl, 0) + lax.ppermute(pick(total, 1 - zl, 0), "zl", SWAP)
    total = total.reshape(2, 12, width)
    total = pick(total, zh, 0) + lax.ppermute(pick(total, 1 - zh, 0), "zh", SWAP)
    flip = [(0, 0), (1, 2), (2, 1), (3, 3)]
    return lax.ppermute(total, ("zh", "c"), flip), sent


def local(
    stream,
    queries,
    new_keys,
    new_values,
    cache_keys,
    cache_values,
    cache_frames,
    group_index,
    timestep,
    gate_table,
    attn_out_weight,
    critic_in,
    critic_cot,
    critic_weight,
):
    zh, x, zl, y, c = (lax.axis_index(a) for a in ("zh", "x", "zl", "y", "c"))
    place = jnp.stack([zl, y, c, zh, x]).astype(jnp.int32)
    near_near, near_far, far_near, far_far = packed(
        place,
        group_index,
        cache_frames,
        (cache_keys[0], new_keys[0], cache_values[0], new_values[0], queries[0]),
    )
    sets = [near_near, lax.ppermute(far_near, "c", SWAP), lax.ppermute(near_far, "zl", SWAP)]
    sets.append(lax.ppermute(lax.ppermute(far_far, "c", SWAP), "zl", SWAP))
    pieces = weight_pieces(critic_weight)

    factor = float(critic_in.shape[0] * 128) ** (-0.5)
    grad_weight, sent = weight_gradient(critic_in, critic_cot, zh, x, zl, y, c, factor)

    own_queries = jnp.concatenate([s[256:288] for s in sets])
    all_queries = [own_queries] + [lax.ppermute(own_queries, "y", turn(k)) for k in (1, 2, 3)]
    *sets, _ = lax.optimization_barrier((*sets, sent))
    partial = attend(sets, all_queries)
    parts = [partial[0]] + [lax.ppermute(partial[k], "y", turn(-k)) for k in (1, 2, 3)]
    mixed = merged(parts)
    cross = [(0, 3), (3, 0), (1, 2), (2, 1)]
    mixed = [
        mixed[0],
        lax.ppermute(mixed[1], "c", SWAP),
        lax.ppermute(mixed[2], "zl", SWAP),
        lax.ppermute(mixed[3], ("zl", "c"), cross),
    ]
    stream_out = streamed(place, timestep, stream[0], gate_table, mixed, attn_out_weight)[None]
    grad_in = grad_of_input(place, critic_cot, pieces)
    return (stream_out, grad_in, grad_weight)


def solution(mesh):
    cut = Mesh(mesh.devices.reshape(2, 4, 2, 4, 2), ("zh", "x", "zl", "y", "c"))
    dp, seq = ("zh", "x"), ("zl", "y", "c")
    whole = dp + seq
    return jax.shard_map(
        local,
        mesh=cut,
        in_specs=(
            P(dp, seq, None),
            P(dp, seq, None),
            P(dp, seq, None),
            P(dp, seq, None),
            P(dp, seq, None),
            P(dp, seq, None),
            P(dp, seq),
            P(dp),
            P(dp),
            P(),
            P(),
            P(whole, None),
            P(whole, None),
            P(whole, None),
        ),
        out_specs=(P(dp, seq, None), P(whole, None), P(whole, None)),
        check_vma=False,
    )
```

```python
import jax
import jax.numpy as jnp
from jax import lax
from jax.experimental import pallas as pl
from jax.experimental.pallas import tpu as pltpu
from jax.sharding import Mesh
from jax.sharding import PartitionSpec as P

HEADS = 12
HEAD = 128
FRAMES_GROUP = 3
WINDOW_FRAMES = 9
BF = jnp.bfloat16
F32 = jnp.float32


SWAP = [(0, 1), (1, 0)]


def turn(k):
    return [(i, (i + k) % 4) for i in range(4)]


def pick(array, index, dim):
    return lax.dynamic_index_in_dim(array, index, dim, keepdims=False)


def in_vmem(x):
    return pltpu.with_memory_space_constraint(x, pltpu.VMEM)


def in_hbm(x):
    return pltpu.with_memory_space_constraint(x, pltpu.HBM)


def room(mebibytes=16, **more):
    return pltpu.CompilerParams(vmem_limit_bytes=mebibytes * 2**20, **more)


def any_spec():
    return pl.BlockSpec(memory_space=pl.ANY)


def scalars():
    return pl.BlockSpec(memory_space=pltpu.SMEM)


def packed(place, group_index, frames, arrays):
    width = arrays[0].shape[1]
    quarter = width // 4
    starts, total = [], 0
    for a in arrays:
        starts.append(total)
        total += a.shape[0]

    def kernel(place_ref, group_ref, frames_ref, *refs):
        ins, outs, live_ref = refs[:5], refs[5:9], refs[9]
        first = FRAMES_GROUP * group_ref[0]
        f = frames_ref[...]
        live_ref[...] = jnp.zeros_like(live_ref)
        live_ref[:, 0:128] = jnp.ones((16, 128), F32)
        alive = (f < first) & (f >= first - WINDOW_FRAMES)
        live_ref[:, 0:96] = jnp.broadcast_to(alive.astype(F32), (16, 96))
        spot = place_ref[2] * 2 + place_ref[0]
        for here in range(4):

            @pl.when(spot == here)
            def _():
                for n, q in enumerate((here, here ^ 1, here ^ 2, here ^ 3)):
                    for a, at in zip(ins, starts):
                        outs[n][at : at + a.shape[0], :] = a[:, q * quarter : (q + 1) * quarter]

        for out in outs:
            out[total : total + 16, :] = live_ref[...].astype(BF)

    return pl.pallas_call(
        kernel,
        out_shape=[jax.ShapeDtypeStruct((total + 16, quarter), BF)] * 4,
        in_specs=[scalars(), scalars()] + [pl.BlockSpec()] * 6,
        scratch_shapes=[pltpu.VMEM((16, quarter), F32)],
        compiler_params=room(),
        name="packed",
    )(place, group_index, frames, *arrays)


def attend(sets, queries):
    quarter = 3 * HEAD

    def kernel(*refs):
        set_refs, query_refs, outs = refs[:4], refs[4:8], refs[8:]
        rows = 128
        lane = lax.broadcasted_iota(jnp.int32, (rows, HEAD), 1)
        alive = jnp.concatenate([r[288:304, 0:128] for r in set_refs], axis=1)
        alive = alive.astype(F32)[0:1, :] > 0.5
        stats = [jnp.zeros((rows, HEAD), F32) for _ in range(4)]
        for h in range(3):
            cols = slice(h * HEAD, (h + 1) * HEAD)
            k = jnp.concatenate([r[0:128, cols] for r in set_refs], axis=0)
            v = jnp.concatenate([r[128:256, cols] for r in set_refs], axis=0)
            for r in range(4):
                s = lax.dot_general(
                    query_refs[r][:, cols], k, (((1,), (1,)), ((), ())), preferred_element_type=F32
                ) * (HEAD ** (-0.5))
                s = jnp.where(alive, s, -1e30)
                top = jnp.max(s, axis=1, keepdims=True).astype(BF).astype(F32)
                w = jnp.where(alive, jnp.exp(s - top), 0.0)
                total = jnp.sum(w, axis=1, keepdims=True)
                o = jnp.dot(w.astype(BF), v, preferred_element_type=F32)
                outs[r][:, cols] = o.astype(BF)
                high = total.astype(BF).astype(F32)
                stats[r] = jnp.where(lane == h, top, stats[r])
                stats[r] = jnp.where(lane == 4 + h, high, stats[r])
                stats[r] = jnp.where(lane == 8 + h, total - high, stats[r])
        for r in range(4):
            outs[r][:, quarter:] = stats[r].astype(BF)

    return pl.pallas_call(
        kernel,
        out_shape=[jax.ShapeDtypeStruct((128, 4 * HEAD), BF)] * 4,
        compiler_params=room(),
        name="attend",
    )(*[in_vmem(a) for a in sets], *[in_vmem(a) for a in queries])


def merged(parts):
    def kernel(*refs):
        ins, outs = refs[:4], refs[4:]
        base = 3 * HEAD
        stats = [r[:, base:].astype(F32) for r in ins]
        for h in range(3):
            tops = [s[:, h : h + 1] for s in stats]
            totals = [s[:, 4 + h : 5 + h] + s[:, 8 + h : 9 + h] for s in stats]
            top = jnp.maximum(jnp.maximum(tops[0], tops[1]), jnp.maximum(tops[2], tops[3]))
            scales = [jnp.exp(t - top) for t in tops]
            total = sum(a * b for a, b in zip(scales, totals))
            cols = slice(h * HEAD, (h + 1) * HEAD)
            summed = sum(r[:, cols].astype(F32) * a for r, a in zip(ins, scales))
            mixed = (summed / total).astype(BF)
            for n in range(4):
                outs[n][:, cols] = mixed[32 * n : 32 * n + 32]

    return pl.pallas_call(
        kernel,
        out_shape=[jax.ShapeDtypeStruct((32, 3 * HEAD), BF)] * 4,
        compiler_params=room(),
        name="merged",
    )(*[in_vmem(a) for a in parts])


def streamed(place, timestep, stream, gate_table, mixed, weight):
    width = weight.shape[1]
    quarter = width // 4

    def kernel(place_ref, step_ref, stream_ref, gate_ref, a_ref, b_ref, c_ref, d_ref, w_ref, out_ref):
        spot = place_ref[2] * 2 + place_ref[0]
        for here in range(4):

            @pl.when(spot == here)
            def _():
                total = jnp.zeros(out_ref.shape, F32)
                for ref, q in zip((a_ref, b_ref, c_ref, d_ref), (here, here ^ 2, here ^ 1, here ^ 3)):
                    total = total + jnp.dot(
                        ref[...], w_ref[q * quarter : (q + 1) * quarter, :], preferred_element_type=F32
                    )
                gate = gate_ref[pl.ds(step_ref[0], 1), :]
                out_ref[...] = (stream_ref[...].astype(F32) + gate * total).astype(BF)

    return pl.pallas_call(
        kernel,
        out_shape=jax.ShapeDtypeStruct(stream.shape, BF),
        in_specs=[scalars(), scalars()] + [pl.BlockSpec()] * 7,
        compiler_params=room(),
        name="streamed",
    )(place, timestep, stream, gate_table, *[in_vmem(a) for a in mixed], weight)


def grad_of_input(place, cot, pieces):
    rows, width = cot.shape
    block = 256
    keys = [k for k, _ in pieces]
    count = len(pieces)

    def kernel(place_ref, cot_ref, *refs):
        ins, (out_ref, buf, weight, sem) = refs[:count], refs[count:]
        zl, y, c, zh, x = (place_ref[n] for n in range(5))

        @pl.when(pl.program_id(0) == 0)
        def _():
            copies = []
            for n, (far, step, other) in enumerate(keys):
                zz = 1 - zl if far else zl
                yy = (y + step) % 4
                cc = 1 - c if other else c
                copies.append(
                    pltpu.make_async_copy(ins[n], buf.at[zz * 8 + yy * 2 + cc], sem.at[n])
                )
                copies[-1].start()
            for copy in copies:
                copy.wait()
            for far in range(2):
                for step in range(4):
                    zz = 1 - zh if far else zh
                    xx = (x + 4 - step) % 4
                    at = 12 * (4 * far + step)
                    for t in range(4):
                        part = [buf[t * 4 + k, at : at + 12, :] for k in range(4)]
                        base = pl.multiple_of(zz * 768 + xx * 192 + t * 48, 16)
                        weight[pl.ds(base, 48), :] = jnp.concatenate(part, axis=0)

        out_ref[...] = lax.dot_general(
            cot_ref[...], weight[...], (((1,), (1,)), ((), ())), preferred_element_type=F32
        ).astype(BF)

    return pl.pallas_call(
        kernel,
        grid=(rows // block,),
        out_shape=jax.ShapeDtypeStruct((rows, width), BF),
        in_specs=[scalars(), pl.BlockSpec((block, width), lambda i: (i, 0))] + [any_spec()] * count,
        out_specs=pl.BlockSpec((block, width), lambda i: (i, 0)),
        scratch_shapes=[
            pltpu.VMEM((16, 96, width), BF),
            pltpu.VMEM((width, width), BF),
            pltpu.SemaphoreType.DMA((count,)),
        ],
        compiler_params=room(28, dimension_semantics=("arbitrary",)),
        name="grad_of_input",
    )(place, cot, *[in_vmem(p) for _, p in pieces])


def joined(arrays):
    rows = [a.shape[0] for a in arrays]

    def kernel(*refs):
        out_ref, at = refs[-1], 0
        for ref, n in zip(refs[:-1], rows):
            out_ref[at : at + n, :] = ref[...]
            at += n

    return pl.pallas_call(
        kernel,
        out_shape=jax.ShapeDtypeStruct((sum(rows), arrays[0].shape[1]), arrays[0].dtype),
        compiler_params=room(),
        name="joined",
    )(*[in_vmem(a) for a in arrays])


def weight_pieces(weight):
    on_x = joined([weight] + [lax.ppermute(weight, "x", turn(k)) for k in (1, 2, 3)])
    near = joined([on_x, lax.ppermute(on_x, "zh", SWAP)])
    far = lax.ppermute(near, "zl", SWAP)
    pieces = {(0, 0): near, (1, 0): far}
    for f in range(2):
        pieces[f, 3] = lax.ppermute(pieces[f, 0], "y", turn(1))
        pieces[f, 1] = lax.ppermute(pieces[f, 0], "y", turn(-1))
    pieces[0, 2] = lax.ppermute(pieces[0, 1], "y", turn(-1))
    pieces[1, 2] = lax.ppermute(pieces[1, 3], "y", turn(1))
    out = [((f, step, 0), p) for (f, step), p in pieces.items()]
    out += [((f, step, 1), lax.ppermute(p, "c", SWAP)) for (f, step), p in pieces.items()]
    return out


def own_queries_of(sets):
    def kernel(*refs):
        for n in range(4):
            refs[4][32 * n : 32 * n + 32, :] = refs[n][256:288, :]

    return pl.pallas_call(
        kernel,
        out_shape=jax.ShapeDtypeStruct((128, 3 * HEAD), BF),
        compiler_params=room(),
        name="own_queries",
    )(*[in_vmem(a) for a in sets])


def product_and_split(place, critic_in, critic_cot, got, factor):
    tokens, width = critic_cot.shape
    half = width // 2

    def kernel(place_ref, in_ref, cot_ref, got_ref, send_l, send_r, keep_l, keep_r):
        x = place_ref[4]
        p = pl.program_id(0)
        result = lax.dot_general(
            in_ref[...], cot_ref[...], (((0,), (0,)), ((), ())), preferred_element_type=F32
        ) * factor + got_ref[...].astype(F32)
        for u in range(2):
            chunk = 2 * p + u
            left = result[192 * u : 192 * u + 192, :half]
            right = result[192 * u : 192 * u + 192, half:]
            kept_l = (chunk == x) | (chunk == 3 - x)
            kept_r = (chunk == x) | (chunk == (x ^ 1))

            @pl.when(kept_l)
            def _():
                keep_l[jnp.where(chunk == x, 0, 1)] = left

            @pl.when(jnp.logical_not(kept_l))
            def _():
                send_l[jnp.where(chunk == (x ^ 1), 0, 1)] = left.astype(BF)

            @pl.when(kept_r)
            def _():
                keep_r[jnp.where(chunk == x, 0, 1)] = right

            @pl.when(jnp.logical_not(kept_r))
            def _():
                send_r[jnp.where(chunk == 3 - x, 0, 1)] = right.astype(BF)

    whole = pl.BlockSpec((2, 192, half), lambda p, place: (0, 0, 0))
    return pl.pallas_call(
        kernel,
        grid_spec=pltpu.PrefetchScalarGridSpec(
            num_scalar_prefetch=1,
            grid=(2,),
            in_specs=[
                pl.BlockSpec((tokens, width // 4), lambda p, place: (0, 2 * place[2] + p)),
                pl.BlockSpec((tokens, width), lambda p, place: (0, 0)),
                pl.BlockSpec((width // 4, width), lambda p, place: (p, 0)),
            ],
            out_specs=[whole] * 4,
        ),
        out_shape=[jax.ShapeDtypeStruct((2, 192, half), BF)] * 2
        + [jax.ShapeDtypeStruct((2, 192, half), F32)] * 2,
        compiler_params=room(40, dimension_semantics=("arbitrary",)),
        name="product_and_split",
    )(place, critic_in, critic_cot, in_hbm(got))


def onward_of(keep_l, keep_r, got_l, got_r):
    def kernel(kl, kr, gl, gr, out_l, out_r):
        out_l[...] = (kl[0] + gl[1].astype(F32)).astype(BF)
        out_r[...] = (kr[0] + gr[1].astype(F32)).astype(BF)

    _, rows, cols = keep_l.shape
    block = pl.BlockSpec((1, rows, cols), lambda i: (1, 0, 0))
    return pl.pallas_call(
        kernel,
        grid=(1,),
        in_specs=[block] * 2 + [pl.BlockSpec(memory_space=pltpu.VMEM)] * 2,
        out_specs=[pl.BlockSpec((rows, cols), lambda i: (0, 0))] * 2,
        out_shape=[jax.ShapeDtypeStruct((rows, cols), BF)] * 2,
        compiler_params=room(),
        name="onward",
    )(keep_l, keep_r, in_vmem(got_l), in_vmem(got_r))


def cut_along_y(place, keep_l, keep_r, got_l, got_r, last_l, last_r):
    half = keep_l.shape[2]

    def kernel(place_ref, kl, kr, gl, gr, ll, lr, own, one, two, three, total):
        total[:, :half] = kl[0] + gl[0].astype(F32) + ll[...].astype(F32)
        total[:, half:] = kr[0] + gr[0].astype(F32) + lr[...].astype(F32)
        y = place_ref[1]
        for k, ref in enumerate((own, one, two, three)):
            at = ((y + k) % 4) * 24
            for z in range(2):
                rows = total[pl.ds(pl.multiple_of(z * 96 + at, 8), 24), :]
                ref[z] = rows.astype(ref.dtype)

    first = pl.BlockSpec((1, 192, half), lambda i: (0, 0, 0))
    out = pl.BlockSpec((2, 24, 2 * half), lambda i: (0, 0, 0))
    return pl.pallas_call(
        kernel,
        grid=(1,),
        in_specs=[scalars()] + [first] * 2 + [pl.BlockSpec(memory_space=pltpu.VMEM)] * 4,
        out_specs=[out] * 4,
        out_shape=[jax.ShapeDtypeStruct((2, 24, 2 * half), F32)]
        + [jax.ShapeDtypeStruct((2, 24, 2 * half), BF)] * 3,
        scratch_shapes=[pltpu.VMEM((192, 2 * half), F32)],
        compiler_params=room(),
        name="cut_along_y",
    )(place, keep_l, keep_r, *[in_vmem(a) for a in (got_l, got_r, last_l, last_r)])


def cut_to_owners(place, own, others):
    width = own.shape[2]

    def kernel(place_ref, own_ref, a, b, d, *outs):
        total = own_ref[...]
        for ref in (a, b, d):
            total = total + ref[...].astype(F32)
        spot = place_ref[0] * 2 + place_ref[3]
        for here in range(4):

            @pl.when(spot == here)
            def _():
                for n in range(4):
                    z, k = (here ^ n) // 2, (here ^ n) % 2
                    outs[n][...] = total[z, 12 * k : 12 * k + 12, :]

    return pl.pallas_call(
        kernel,
        in_specs=[scalars()] + [pl.BlockSpec()] * 4,
        out_shape=[jax.ShapeDtypeStruct((12, width), F32)] * 4,
        compiler_params=room(),
        name="cut_to_owners",
    )(place, own, *[in_vmem(a) for a in others])


def added(arrays):
    def kernel(*refs):
        refs[-1][...] = (refs[0][...] + refs[1][...]) + (refs[2][...] + refs[3][...])

    return pl.pallas_call(
        kernel,
        out_shape=jax.ShapeDtypeStruct(arrays[0].shape, F32),
        compiler_params=room(),
        name="added",
    )(*[in_vmem(a) for a in arrays])


def weight_gradient(place, critic_in, critic_cot, c, factor):
    half = critic_cot.shape[1] // 2
    theirs = lax.dynamic_slice_in_dim(critic_in, (1 - c) * half, half, 1)
    theirs = (
        lax.dot_general(theirs, critic_cot, (((0,), (0,)), ((), ())), preferred_element_type=F32)
        * factor
    ).astype(BF)
    got = lax.ppermute(theirs, "c", SWAP)
    send_l, send_r, keep_l, keep_r = product_and_split(place, critic_in, critic_cot, got, factor)
    near = [(0, 1), (1, 0), (2, 3), (3, 2)]
    wrap = [(0, 3), (3, 0), (1, 2), (2, 1)]
    got_l = lax.ppermute(send_l, "x", near)
    got_r = lax.ppermute(send_r, "x", wrap)
    on_l, on_r = onward_of(keep_l, keep_r, got_l, got_r)
    last_l = lax.ppermute(on_l, "x", wrap)
    last_r = lax.ppermute(on_r, "x", near)
    own, *others = cut_along_y(place, keep_l, keep_r, got_l, got_r, last_l, last_r)
    others = [lax.ppermute(a, "y", turn(k)) for a, k in zip(others, (1, 2, 3))]
    cuts = cut_to_owners(place, own, others)

    def owner(far_z, far_c):
        spots = [(h, z, k) for h in range(2) for z in range(2) for k in range(2)]
        return [(h * 4 + z * 2 + k, k * 4 + (z ^ far_z) * 2 + (h ^ far_c)) for h, z, k in spots]

    ends = [
        lax.ppermute(a, ("zh", "zl", "c"), owner(n // 2, n % 2)) for n, a in enumerate(cuts)
    ]
    return added(ends), send_l


def local(
    stream,
    queries,
    new_keys,
    new_values,
    cache_keys,
    cache_values,
    cache_frames,
    group_index,
    timestep,
    gate_table,
    attn_out_weight,
    critic_in,
    critic_cot,
    critic_weight,
):
    zh, x, zl, y, c = (lax.axis_index(a) for a in ("zh", "x", "zl", "y", "c"))
    place = jnp.stack([zl, y, c, zh, x]).astype(jnp.int32)
    near_near, near_far, far_near, far_far = packed(
        place,
        group_index,
        cache_frames,
        (cache_keys[0], new_keys[0], cache_values[0], new_values[0], queries[0]),
    )
    sets = [near_near, lax.ppermute(far_near, "c", SWAP), lax.ppermute(near_far, "zl", SWAP)]
    sets.append(lax.ppermute(lax.ppermute(far_far, "c", SWAP), "zl", SWAP))
    pieces = weight_pieces(critic_weight)

    factor = float(critic_in.shape[0] * 128) ** (-0.5)
    grad_weight, sent = weight_gradient(place, critic_in, critic_cot, c, factor)

    own_queries = own_queries_of(sets)
    all_queries = [own_queries] + [lax.ppermute(own_queries, "y", turn(k)) for k in (1, 2, 3)]
    *sets, _ = lax.optimization_barrier((*sets, sent))
    partial = attend(sets, all_queries)
    parts = [partial[0]] + [lax.ppermute(partial[k], "y", turn(-k)) for k in (1, 2, 3)]
    mixed = merged(parts)
    cross = [(0, 3), (3, 0), (1, 2), (2, 1)]
    mixed = [
        mixed[0],
        lax.ppermute(mixed[1], "c", SWAP),
        lax.ppermute(mixed[2], "zl", SWAP),
        lax.ppermute(mixed[3], ("zl", "c"), cross),
    ]
    stream_out = streamed(place, timestep, stream[0], gate_table, mixed, attn_out_weight)[None]
    grad_in = grad_of_input(place, critic_cot, pieces)
    return (stream_out, grad_in, grad_weight)


def solution(mesh):
    cut = Mesh(mesh.devices.reshape(2, 4, 2, 4, 2), ("zh", "x", "zl", "y", "c"))
    dp, seq = ("zh", "x"), ("zl", "y", "c")
    whole = dp + seq
    return jax.shard_map(
        local,
        mesh=cut,
        in_specs=(
            P(dp, seq, None),
            P(dp, seq, None),
            P(dp, seq, None),
            P(dp, seq, None),
            P(dp, seq, None),
            P(dp, seq, None),
            P(dp, seq),
            P(dp),
            P(dp),
            P(),
            P(),
            P(whole, None),
            P(whole, None),
            P(whole, None),
        ),
        out_specs=(P(dp, seq, None), P(whole, None), P(whole, None)),
        check_vma=False,
    )
```

```python
import jax
import jax.numpy as jnp
from jax import lax
from jax.experimental import pallas as pl
from jax.experimental.pallas import tpu as pltpu
from jax.sharding import Mesh
from jax.sharding import PartitionSpec as P

HEAD = 128
FRAMES_GROUP = 3
WINDOW_FRAMES = 9
BF = jnp.bfloat16
F32 = jnp.float32


SWAP = [(0, 1), (1, 0)]


def turn(k):
    return [(i, (i + k) % 4) for i in range(4)]


def in_vmem(x):
    return pltpu.with_memory_space_constraint(x, pltpu.VMEM)


def in_hbm(x):
    return pltpu.with_memory_space_constraint(x, pltpu.HBM)


def room(mebibytes=16, **more):
    return pltpu.CompilerParams(vmem_limit_bytes=mebibytes * 2**20, **more)


def any_spec():
    return pl.BlockSpec(memory_space=pl.ANY)


def scalars():
    return pl.BlockSpec(memory_space=pltpu.SMEM)


def packed(place, group_index, frames, arrays):
    width = arrays[0].shape[1]
    quarter = width // 4
    starts, total = [], 0
    for a in arrays:
        starts.append(total)
        total += a.shape[0]

    def kernel(place_ref, group_ref, frames_ref, *refs):
        ins, outs, live_ref = refs[:5], refs[5:9], refs[9]
        first = FRAMES_GROUP * group_ref[0]
        f = frames_ref[...]
        live_ref[...] = jnp.zeros_like(live_ref)
        live_ref[:, 0:128] = jnp.ones((16, 128), F32)
        alive = (f < first) & (f >= first - WINDOW_FRAMES)
        live_ref[:, 0:96] = jnp.broadcast_to(alive.astype(F32), (16, 96))
        spot = place_ref[2] * 2 + place_ref[0]
        for here in range(4):

            @pl.when(spot == here)
            def _():
                for n, q in enumerate((here, here ^ 1, here ^ 2, here ^ 3)):
                    for a, at in zip(ins, starts):
                        outs[n][at : at + a.shape[0], :] = a[:, q * quarter : (q + 1) * quarter]

        for out in outs:
            out[total : total + 16, :] = live_ref[...].astype(BF)

    return pl.pallas_call(
        kernel,
        out_shape=[jax.ShapeDtypeStruct((total + 16, quarter), BF)] * 4,
        in_specs=[scalars(), scalars()] + [pl.BlockSpec()] * 6,
        scratch_shapes=[pltpu.VMEM((16, quarter), F32)],
        compiler_params=room(),
        name="packed",
    )(place, group_index, frames, *[in_hbm(a) for a in arrays])


def attend(sets, queries):
    quarter = 3 * HEAD

    def kernel(*refs):
        set_refs, query_refs, outs = refs[:4], refs[4:8], refs[8:]
        rows = 128
        lane = lax.broadcasted_iota(jnp.int32, (rows, HEAD), 1)
        alive = jnp.concatenate([r[288:304, 0:128] for r in set_refs], axis=1)
        alive = alive.astype(F32)[0:1, :] > 0.5
        stats = [jnp.zeros((rows, HEAD), F32) for _ in range(4)]
        for h in range(3):
            cols = slice(h * HEAD, (h + 1) * HEAD)
            k = jnp.concatenate([r[0:128, cols] for r in set_refs], axis=0)
            v = jnp.concatenate([r[128:256, cols] for r in set_refs], axis=0)
            for r in range(4):
                s = lax.dot_general(
                    query_refs[r][:, cols], k, (((1,), (1,)), ((), ())), preferred_element_type=F32
                ) * (HEAD ** (-0.5))
                s = jnp.where(alive, s, -1e30)
                top = jnp.max(s, axis=1, keepdims=True).astype(BF).astype(F32)
                w = jnp.where(alive, jnp.exp(s - top), 0.0)
                total = jnp.sum(w, axis=1, keepdims=True)
                o = jnp.dot(w.astype(BF), v, preferred_element_type=F32)
                outs[r][:, cols] = o.astype(BF)
                high = total.astype(BF).astype(F32)
                stats[r] = jnp.where(lane == h, top, stats[r])
                stats[r] = jnp.where(lane == 4 + h, high, stats[r])
                stats[r] = jnp.where(lane == 8 + h, total - high, stats[r])
        for r in range(4):
            outs[r][:, quarter:] = stats[r].astype(BF)

    return pl.pallas_call(
        kernel,
        out_shape=[jax.ShapeDtypeStruct((128, 4 * HEAD), BF)] * 4,
        compiler_params=room(),
        name="attend",
    )(*[in_vmem(a) for a in sets], *[in_vmem(a) for a in queries])


def merged(parts):
    def kernel(*refs):
        ins, outs = refs[:4], refs[4:]
        base = 3 * HEAD
        stats = [r[:, base:].astype(F32) for r in ins]
        for h in range(3):
            tops = [s[:, h : h + 1] for s in stats]
            totals = [s[:, 4 + h : 5 + h] + s[:, 8 + h : 9 + h] for s in stats]
            top = jnp.maximum(jnp.maximum(tops[0], tops[1]), jnp.maximum(tops[2], tops[3]))
            scales = [jnp.exp(t - top) for t in tops]
            total = sum(a * b for a, b in zip(scales, totals))
            cols = slice(h * HEAD, (h + 1) * HEAD)
            summed = sum(r[:, cols].astype(F32) * a for r, a in zip(ins, scales))
            mixed = (summed / total).astype(BF)
            for n in range(4):
                outs[n][:, cols] = mixed[32 * n : 32 * n + 32]

    return pl.pallas_call(
        kernel,
        out_shape=[jax.ShapeDtypeStruct((32, 3 * HEAD), BF)] * 4,
        compiler_params=room(),
        name="merged",
    )(*[in_vmem(a) for a in parts])


def streamed(place, timestep, stream, gate_table, mixed, weight):
    width = weight.shape[1]
    quarter = width // 4

    def kernel(place_ref, step_ref, stream_ref, gate_ref, a_ref, b_ref, c_ref, d_ref, w_ref, out_ref):
        spot = place_ref[2] * 2 + place_ref[0]
        for here in range(4):

            @pl.when(spot == here)
            def _():
                total = jnp.zeros(out_ref.shape, F32)
                for ref, q in zip((a_ref, b_ref, c_ref, d_ref), (here, here ^ 2, here ^ 1, here ^ 3)):
                    total = total + jnp.dot(
                        ref[...], w_ref[q * quarter : (q + 1) * quarter, :], preferred_element_type=F32
                    )
                gate = gate_ref[pl.ds(step_ref[0], 1), :]
                out_ref[...] = (stream_ref[...].astype(F32) + gate * total).astype(BF)

    return pl.pallas_call(
        kernel,
        out_shape=jax.ShapeDtypeStruct(stream.shape, BF),
        in_specs=[scalars(), scalars()] + [pl.BlockSpec()] * 7,
        compiler_params=room(),
        name="streamed",
    )(place, timestep, stream, gate_table, *[in_vmem(a) for a in mixed], weight)


def grad_of_input(place, cot, pieces):
    rows, width = cot.shape
    block = 256
    keys = [k for k, _ in pieces]
    count = len(pieces)

    def kernel(place_ref, cot_ref, *refs):
        ins, (out_ref, buf, weight, sem) = refs[:count], refs[count:]
        zl, y, c, zh, x = (place_ref[n] for n in range(5))

        @pl.when(pl.program_id(0) == 0)
        def _():
            copies = []
            for n, (far, step, other) in enumerate(keys):
                zz = 1 - zl if far else zl
                yy = (y + step) % 4
                cc = 1 - c if other else c
                copies.append(
                    pltpu.make_async_copy(ins[n], buf.at[zz * 8 + yy * 2 + cc], sem.at[n])
                )
                copies[-1].start()
            for copy in copies:
                copy.wait()
            for far in range(2):
                for step in range(4):
                    zz = 1 - zh if far else zh
                    xx = (x + 4 - step) % 4
                    at = 12 * (4 * far + step)
                    for t in range(4):
                        part = [buf[t * 4 + k, at : at + 12, :] for k in range(4)]
                        base = pl.multiple_of(zz * 768 + xx * 192 + t * 48, 16)
                        weight[pl.ds(base, 48), :] = jnp.concatenate(part, axis=0)

        out_ref[...] = lax.dot_general(
            cot_ref[...], weight[...], (((1,), (1,)), ((), ())), preferred_element_type=F32
        ).astype(BF)

    return pl.pallas_call(
        kernel,
        grid=(rows // block,),
        out_shape=jax.ShapeDtypeStruct((rows, width), BF),
        in_specs=[scalars(), pl.BlockSpec((block, width), lambda i: (i, 0))] + [any_spec()] * count,
        out_specs=pl.BlockSpec((block, width), lambda i: (i, 0)),
        scratch_shapes=[
            pltpu.VMEM((16, 96, width), BF),
            pltpu.VMEM((width, width), BF),
            pltpu.SemaphoreType.DMA((count,)),
        ],
        compiler_params=room(28, dimension_semantics=("arbitrary",)),
        name="grad_of_input",
    )(place, cot, *[in_vmem(p) for _, p in pieces])


def joined(arrays):
    rows = [a.shape[0] for a in arrays]

    def kernel(*refs):
        out_ref, at = refs[-1], 0
        for ref, n in zip(refs[:-1], rows):
            out_ref[at : at + n, :] = ref[...]
            at += n

    return pl.pallas_call(
        kernel,
        out_shape=jax.ShapeDtypeStruct((sum(rows), arrays[0].shape[1]), arrays[0].dtype),
        compiler_params=room(),
        name="joined",
    )(in_hbm(arrays[0]), *[in_vmem(a) for a in arrays[1:]])


def weight_pieces(weight):
    on_x = [weight] + [lax.ppermute(weight, "x", turn(k)) for k in (1, 2, 3)]
    on_x = joined(on_x)
    far = lax.ppermute(on_x, "zh", SWAP)
    near = joined([on_x, far])
    far = lax.ppermute(near, "zl", SWAP)
    pieces = {(0, 0): near, (1, 0): far}
    for f in range(2):
        pieces[f, 3] = lax.ppermute(pieces[f, 0], "y", turn(1))
        pieces[f, 1] = lax.ppermute(pieces[f, 0], "y", turn(-1))
    pieces[0, 2] = lax.ppermute(pieces[0, 1], "y", turn(-1))
    pieces[1, 2] = lax.ppermute(pieces[1, 3], "y", turn(1))
    out = [((f, step, 0), p) for (f, step), p in pieces.items()]
    out += [((f, step, 1), lax.ppermute(p, "c", SWAP)) for (f, step), p in pieces.items()]
    return out


def own_queries_of(sets):
    def kernel(*refs):
        for n in range(4):
            refs[4][32 * n : 32 * n + 32, :] = refs[n][256:288, :]

    return pl.pallas_call(
        kernel,
        out_shape=jax.ShapeDtypeStruct((128, 3 * HEAD), BF),
        compiler_params=room(),
        name="own_queries",
    )(*[in_vmem(a) for a in sets])


def product_and_split(place, critic_in, critic_cot, got, factor):
    tokens, width = critic_cot.shape
    half = width // 2

    def kernel(place_ref, in_ref, cot_ref, got_ref, send_l, send_r, keep_l, keep_r):
        x = place_ref[4]
        p = pl.program_id(0)
        result = lax.dot_general(
            in_ref[...], cot_ref[...], (((0,), (0,)), ((), ())), preferred_element_type=F32
        ) * factor + got_ref[...].astype(F32)
        for u in range(2):
            chunk = 2 * p + u
            left = result[192 * u : 192 * u + 192, :half]
            right = result[192 * u : 192 * u + 192, half:]
            kept_l = (chunk == x) | (chunk == 3 - x)
            kept_r = (chunk == x) | (chunk == (x ^ 1))

            @pl.when(kept_l)
            def _():
                keep_l[jnp.where(chunk == x, 0, 1)] = left

            @pl.when(jnp.logical_not(kept_l))
            def _():
                send_l[jnp.where(chunk == (x ^ 1), 0, 1)] = left.astype(BF)

            @pl.when(kept_r)
            def _():
                keep_r[jnp.where(chunk == x, 0, 1)] = right

            @pl.when(jnp.logical_not(kept_r))
            def _():
                send_r[jnp.where(chunk == 3 - x, 0, 1)] = right.astype(BF)

    whole = pl.BlockSpec((2, 192, half), lambda p, place: (0, 0, 0))
    return pl.pallas_call(
        kernel,
        grid_spec=pltpu.PrefetchScalarGridSpec(
            num_scalar_prefetch=1,
            grid=(2,),
            in_specs=[
                pl.BlockSpec((tokens, width // 4), lambda p, place: (0, 2 * place[2] + p)),
                pl.BlockSpec((tokens, width), lambda p, place: (0, 0)),
                pl.BlockSpec((width // 4, width), lambda p, place: (p, 0)),
            ],
            out_specs=[whole] * 4,
        ),
        out_shape=[jax.ShapeDtypeStruct((2, 192, half), BF)] * 2
        + [jax.ShapeDtypeStruct((2, 192, half), F32)] * 2,
        compiler_params=room(40, dimension_semantics=("arbitrary",)),
        name="product_and_split",
    )(place, in_hbm(critic_in), critic_cot, in_vmem(got))


def onward_of(keep_l, keep_r, got_l, got_r):
    def kernel(kl, kr, gl, gr, out_l, out_r):
        out_l[...] = (kl[0] + gl[1].astype(F32)).astype(BF)
        out_r[...] = (kr[0] + gr[1].astype(F32)).astype(BF)

    _, rows, cols = keep_l.shape
    block = pl.BlockSpec((1, rows, cols), lambda i: (1, 0, 0))
    return pl.pallas_call(
        kernel,
        grid=(1,),
        in_specs=[block] * 2 + [pl.BlockSpec(memory_space=pltpu.VMEM)] * 2,
        out_specs=[pl.BlockSpec((rows, cols), lambda i: (0, 0))] * 2,
        out_shape=[jax.ShapeDtypeStruct((rows, cols), BF)] * 2,
        compiler_params=room(),
        name="onward",
    )(keep_l, keep_r, in_vmem(got_l), in_vmem(got_r))


def cut_along_y(place, keep_l, keep_r, got_l, got_r, last_l, last_r):
    half = keep_l.shape[2]

    def kernel(place_ref, kl, kr, gl, gr, ll, lr, own, one, two, three, total):
        total[:, :half] = kl[0] + gl[0].astype(F32) + ll[...].astype(F32)
        total[:, half:] = kr[0] + gr[0].astype(F32) + lr[...].astype(F32)
        y = place_ref[1]
        for k, ref in enumerate((own, one, two, three)):
            at = ((y + k) % 4) * 24
            for z in range(2):
                rows = total[pl.ds(pl.multiple_of(z * 96 + at, 8), 24), :]
                ref[z] = rows.astype(ref.dtype)

    first = pl.BlockSpec((1, 192, half), lambda i: (0, 0, 0))
    out = pl.BlockSpec((2, 24, 2 * half), lambda i: (0, 0, 0))
    return pl.pallas_call(
        kernel,
        grid=(1,),
        in_specs=[scalars()] + [first] * 2 + [pl.BlockSpec(memory_space=pltpu.VMEM)] * 4,
        out_specs=[out] * 4,
        out_shape=[jax.ShapeDtypeStruct((2, 24, 2 * half), F32)]
        + [jax.ShapeDtypeStruct((2, 24, 2 * half), BF)] * 3,
        scratch_shapes=[pltpu.VMEM((192, 2 * half), F32)],
        compiler_params=room(),
        name="cut_along_y",
    )(place, keep_l, keep_r, *[in_vmem(a) for a in (got_l, got_r, last_l, last_r)])


def cut_to_owners(place, own, others):
    width = own.shape[2]

    def kernel(place_ref, own_ref, a, b, d, *outs):
        total = own_ref[...]
        for ref in (a, b, d):
            total = total + ref[...].astype(F32)
        spot = place_ref[0] * 2 + place_ref[3]
        for here in range(4):

            @pl.when(spot == here)
            def _():
                for n in range(4):
                    z, k = (here ^ n) // 2, (here ^ n) % 2
                    outs[n][...] = total[z, 12 * k : 12 * k + 12, :]

    return pl.pallas_call(
        kernel,
        in_specs=[scalars()] + [pl.BlockSpec()] * 4,
        out_shape=[jax.ShapeDtypeStruct((12, width), F32)] * 4,
        compiler_params=room(),
        name="cut_to_owners",
    )(place, own, *[in_vmem(a) for a in others])


def added(arrays):
    def kernel(*refs):
        refs[-1][...] = (refs[0][...] + refs[1][...]) + (refs[2][...] + refs[3][...])

    return pl.pallas_call(
        kernel,
        out_shape=jax.ShapeDtypeStruct(arrays[0].shape, F32),
        compiler_params=room(),
        name="added",
    )(*[in_vmem(a) for a in arrays])


def weight_gradient(place, critic_in, critic_cot, c, factor):
    half = critic_cot.shape[1] // 2
    theirs = lax.dynamic_slice_in_dim(critic_in, (1 - c) * half, half, 1)
    theirs = (
        lax.dot_general(
            theirs, critic_cot, (((0,), (0,)), ((), ())), preferred_element_type=F32
        )
        * factor
    ).astype(BF)
    got = lax.ppermute(theirs, "c", SWAP)
    send_l, send_r, keep_l, keep_r = product_and_split(place, critic_in, critic_cot, got, factor)
    near = [(0, 1), (1, 0), (2, 3), (3, 2)]
    wrap = [(0, 3), (3, 0), (1, 2), (2, 1)]
    got_l = lax.ppermute(send_l, "x", near)
    got_r = lax.ppermute(send_r, "x", wrap)
    on_l, on_r = onward_of(keep_l, keep_r, got_l, got_r)
    last_l = lax.ppermute(on_l, "x", wrap)
    last_r = lax.ppermute(on_r, "x", near)
    own, *others = cut_along_y(place, keep_l, keep_r, got_l, got_r, last_l, last_r)
    others = [lax.ppermute(a, "y", turn(k)) for a, k in zip(others, (1, 2, 3))]
    cuts = cut_to_owners(place, own, others)

    def owner(far_z, far_c):
        spots = [(h, z, k) for h in range(2) for z in range(2) for k in range(2)]
        return [(h * 4 + z * 2 + k, k * 4 + (z ^ far_z) * 2 + (h ^ far_c)) for h, z, k in spots]

    ends = [lax.ppermute(a, ("zh", "zl", "c"), owner(n // 2, n % 2)) for n, a in enumerate(cuts)]
    return added(ends)


def step(
    stream,
    queries,
    new_keys,
    new_values,
    cache_keys,
    cache_values,
    cache_frames,
    group_index,
    timestep,
    gate_table,
    attn_out_weight,
    critic_in,
    critic_cot,
    critic_weight,
):
    zh, x, zl, y, c = (lax.axis_index(a) for a in ("zh", "x", "zl", "y", "c"))
    place = jnp.stack([zl, y, c, zh, x]).astype(jnp.int32)
    near_near, near_far, far_near, far_far = packed(
        place,
        group_index,
        cache_frames,
        (cache_keys[0], new_keys[0], cache_values[0], new_values[0], queries[0]),
    )
    sets = [near_near, lax.ppermute(far_near, "c", SWAP), lax.ppermute(near_far, "zl", SWAP)]
    sets.append(lax.ppermute(lax.ppermute(far_far, "c", SWAP), "zl", SWAP))
    pieces = weight_pieces(critic_weight)

    factor = float(critic_in.shape[0] * 128) ** (-0.5)
    grad_weight = weight_gradient(place, critic_in, critic_cot, c, factor)

    own = own_queries_of(sets)
    all_queries = [own] + [lax.ppermute(own, "y", turn(k)) for k in (1, 2, 3)]
    partial = attend(sets, all_queries)
    parts = [partial[0]] + [lax.ppermute(partial[k], "y", turn(-k)) for k in (1, 2, 3)]
    mixed = merged(parts)
    cross = [(0, 3), (3, 0), (1, 2), (2, 1)]
    mixed = [
        mixed[0],
        lax.ppermute(mixed[1], "c", SWAP),
        lax.ppermute(mixed[2], "zl", SWAP),
        lax.ppermute(mixed[3], ("zl", "c"), cross),
    ]
    stream_out = streamed(place, timestep, stream[0], gate_table, mixed, attn_out_weight)[None]
    grad_in = grad_of_input(place, critic_cot, pieces)
    return (stream_out, grad_in, grad_weight)


def solution(mesh):
    cut = Mesh(mesh.devices.reshape(2, 4, 2, 4, 2), ("zh", "x", "zl", "y", "c"))
    dp, seq = ("zh", "x"), ("zl", "y", "c")
    whole = dp + seq
    return jax.shard_map(
        step,
        mesh=cut,
        in_specs=(
            P(dp, seq, None),
            P(dp, seq, None),
            P(dp, seq, None),
            P(dp, seq, None),
            P(dp, seq, None),
            P(dp, seq, None),
            P(dp, seq),
            P(dp),
            P(dp),
            P(),
            P(),
            P(whole, None),
            P(whole, None),
            P(whole, None),
        ),
        out_specs=(P(dp, seq, None), P(whole, None), P(whole, None)),
        check_vma=False,
    )
```

```python
import jax
import jax.numpy as jnp
from jax import lax
from jax.experimental import pallas as pl
from jax.experimental.pallas import tpu as pltpu
from jax.sharding import Mesh
from jax.sharding import PartitionSpec as P

HEAD = 128
FRAMES_GROUP = 3
WINDOW_FRAMES = 9
BF = jnp.bfloat16
F32 = jnp.float32


SWAP = [(0, 1), (1, 0)]


def turn(k):
    return [(i, (i + k) % 4) for i in range(4)]


def in_vmem(x):
    return pltpu.with_memory_space_constraint(x, pltpu.VMEM)


def in_hbm(x):
    return pltpu.with_memory_space_constraint(x, pltpu.HBM)


def room(mebibytes=16, **more):
    return pltpu.CompilerParams(vmem_limit_bytes=mebibytes * 2**20, **more)


def any_spec():
    return pl.BlockSpec(memory_space=pl.ANY)


def scalars():
    return pl.BlockSpec(memory_space=pltpu.SMEM)


def packed(place, group_index, frames, arrays):
    width = arrays[0].shape[1]
    quarter = width // 4
    starts, total = [], 0
    for a in arrays:
        starts.append(total)
        total += a.shape[0]

    def kernel(place_ref, group_ref, frames_ref, *refs):
        ins, outs, live_ref = refs[:5], refs[5:9], refs[9]
        first = FRAMES_GROUP * group_ref[0]
        f = frames_ref[...]
        live_ref[...] = jnp.zeros_like(live_ref)
        live_ref[:, 0:128] = jnp.ones((16, 128), F32)
        alive = (f < first) & (f >= first - WINDOW_FRAMES)
        live_ref[:, 0:96] = jnp.broadcast_to(alive.astype(F32), (16, 96))
        spot = place_ref[2] * 2 + place_ref[0]
        for here in range(4):

            @pl.when(spot == here)
            def _():
                for n, q in enumerate((here, here ^ 1, here ^ 2, here ^ 3)):
                    for a, at in zip(ins, starts):
                        outs[n][at : at + a.shape[0], :] = a[:, q * quarter : (q + 1) * quarter]

        for out in outs:
            out[total : total + 16, :] = live_ref[...].astype(BF)

    return pl.pallas_call(
        kernel,
        out_shape=[jax.ShapeDtypeStruct((total + 16, quarter), BF)] * 4,
        in_specs=[scalars(), scalars()] + [pl.BlockSpec()] * 6,
        scratch_shapes=[pltpu.VMEM((16, quarter), F32)],
        compiler_params=room(),
        name="packed",
    )(place, group_index, frames, *[in_hbm(a) for a in arrays])


def attend(sets, queries):
    quarter = 3 * HEAD

    def kernel(*refs):
        set_refs, query_refs, outs = refs[:4], refs[4:8], refs[8:]
        rows = 128
        lane = lax.broadcasted_iota(jnp.int32, (rows, HEAD), 1)
        alive = jnp.concatenate([r[288:304, 0:128] for r in set_refs], axis=1)
        alive = alive.astype(F32)[0:1, :] > 0.5
        stats = [jnp.zeros((rows, HEAD), F32) for _ in range(4)]
        for h in range(3):
            cols = slice(h * HEAD, (h + 1) * HEAD)
            k = jnp.concatenate([r[0:128, cols] for r in set_refs], axis=0)
            v = jnp.concatenate([r[128:256, cols] for r in set_refs], axis=0)
            for r in range(4):
                s = lax.dot_general(
                    query_refs[r][:, cols], k, (((1,), (1,)), ((), ())), preferred_element_type=F32
                ) * (HEAD ** (-0.5))
                s = jnp.where(alive, s, -1e30)
                top = jnp.max(s, axis=1, keepdims=True).astype(BF).astype(F32)
                w = jnp.exp(s - top)
                total = jnp.sum(w, axis=1, keepdims=True)
                o = jnp.dot(w.astype(BF), v, preferred_element_type=F32)
                outs[r][:, cols] = o.astype(BF)
                high = total.astype(BF).astype(F32)
                stats[r] = jnp.where(lane == h, top, stats[r])
                stats[r] = jnp.where(lane == 4 + h, high, stats[r])
                stats[r] = jnp.where(lane == 8 + h, total - high, stats[r])
        for r in range(4):
            outs[r][:, quarter:] = stats[r].astype(BF)

    return pl.pallas_call(
        kernel,
        out_shape=[jax.ShapeDtypeStruct((128, 4 * HEAD), BF)] * 4,
        compiler_params=room(),
        name="attend",
    )(*[in_vmem(a) for a in sets], *[in_vmem(a) for a in queries])


def merged(parts):
    def kernel(*refs):
        ins, outs = refs[:4], refs[4:]
        base = 3 * HEAD
        stats = [r[:, base:].astype(F32) for r in ins]
        for h in range(3):
            tops = [s[:, h : h + 1] for s in stats]
            totals = [s[:, 4 + h : 5 + h] + s[:, 8 + h : 9 + h] for s in stats]
            top = jnp.maximum(jnp.maximum(tops[0], tops[1]), jnp.maximum(tops[2], tops[3]))
            scales = [jnp.exp(t - top) for t in tops]
            total = sum(a * b for a, b in zip(scales, totals))
            cols = slice(h * HEAD, (h + 1) * HEAD)
            summed = sum(r[:, cols].astype(F32) * a for r, a in zip(ins, scales))
            mixed = (summed / total).astype(BF)
            for n in range(4):
                outs[n][:, cols] = mixed[32 * n : 32 * n + 32]

    return pl.pallas_call(
        kernel,
        out_shape=[jax.ShapeDtypeStruct((32, 3 * HEAD), BF)] * 4,
        compiler_params=room(),
        name="merged",
    )(*[in_vmem(a) for a in parts])


def streamed(place, timestep, stream, gate_table, mixed, weight):
    width = weight.shape[1]
    quarter = width // 4

    def kernel(place_ref, step_ref, stream_ref, gate_ref, a_ref, b_ref, c_ref, d_ref, w_ref, out_ref):
        spot = place_ref[2] * 2 + place_ref[0]
        for here in range(4):

            @pl.when(spot == here)
            def _():
                total = jnp.zeros(out_ref.shape, F32)
                for ref, q in zip((a_ref, b_ref, c_ref, d_ref), (here, here ^ 2, here ^ 1, here ^ 3)):
                    total = total + jnp.dot(
                        ref[...], w_ref[q * quarter : (q + 1) * quarter, :], preferred_element_type=F32
                    )
                gate = gate_ref[pl.ds(step_ref[0], 1), :]
                out_ref[...] = (stream_ref[...].astype(F32) + gate * total).astype(BF)

    return pl.pallas_call(
        kernel,
        out_shape=jax.ShapeDtypeStruct(stream.shape, BF),
        in_specs=[scalars(), scalars()] + [pl.BlockSpec()] * 7,
        compiler_params=room(),
        name="streamed",
    )(place, timestep, stream, gate_table, *[in_vmem(a) for a in mixed], weight)


def grad_of_input(place, cot, pieces):
    rows, width = cot.shape
    block = 256
    keys = [k for k, _ in pieces]
    count = len(pieces)

    def kernel(place_ref, cot_ref, *refs):
        ins, (out_ref, buf, weight, sem) = refs[:count], refs[count:]
        zl, y, c, zh, x = (place_ref[n] for n in range(5))

        @pl.when(pl.program_id(0) == 0)
        def _():
            copies = []
            for n, (far, step, other) in enumerate(keys):
                zz = 1 - zl if far else zl
                yy = (y + step) % 4
                cc = 1 - c if other else c
                copies.append(
                    pltpu.make_async_copy(ins[n], buf.at[zz * 8 + yy * 2 + cc], sem.at[n])
                )
                copies[-1].start()
            for copy in copies:
                copy.wait()
            for far in range(2):
                for step in range(4):
                    zz = 1 - zh if far else zh
                    xx = (x + 4 - step) % 4
                    at = 12 * (4 * far + step)
                    for t in range(4):
                        part = [buf[t * 4 + k, at : at + 12, :] for k in range(4)]
                        base = pl.multiple_of(zz * 768 + xx * 192 + t * 48, 16)
                        weight[pl.ds(base, 48), :] = jnp.concatenate(part, axis=0)

        out_ref[...] = lax.dot_general(
            cot_ref[...], weight[...], (((1,), (1,)), ((), ())), preferred_element_type=F32
        ).astype(BF)

    return pl.pallas_call(
        kernel,
        grid=(rows // block,),
        out_shape=jax.ShapeDtypeStruct((rows, width), BF),
        in_specs=[scalars(), pl.BlockSpec((block, width), lambda i: (i, 0))] + [any_spec()] * count,
        out_specs=pl.BlockSpec((block, width), lambda i: (i, 0)),
        scratch_shapes=[
            pltpu.VMEM((16, 96, width), BF),
            pltpu.VMEM((width, width), BF),
            pltpu.SemaphoreType.DMA((count,)),
        ],
        compiler_params=room(28, dimension_semantics=("arbitrary",)),
        name="grad_of_input",
    )(place, cot, *[in_vmem(p) for _, p in pieces])


def joined(arrays):
    rows = [a.shape[0] for a in arrays]

    def kernel(*refs):
        out_ref, at = refs[-1], 0
        for ref, n in zip(refs[:-1], rows):
            out_ref[at : at + n, :] = ref[...]
            at += n

    return pl.pallas_call(
        kernel,
        out_shape=jax.ShapeDtypeStruct((sum(rows), arrays[0].shape[1]), arrays[0].dtype),
        compiler_params=room(),
        name="joined",
    )(in_hbm(arrays[0]), *[in_vmem(a) for a in arrays[1:]])


def weight_pieces(weight):
    on_x = [weight] + [lax.ppermute(weight, "x", turn(k)) for k in (1, 2, 3)]
    on_x = joined(on_x)
    far = lax.ppermute(on_x, "zh", SWAP)
    near = joined([on_x, far])
    far = lax.ppermute(near, "zl", SWAP)
    pieces = {(0, 0): near, (1, 0): far}
    for f in range(2):
        pieces[f, 3] = lax.ppermute(pieces[f, 0], "y", turn(1))
        pieces[f, 1] = lax.ppermute(pieces[f, 0], "y", turn(-1))
    pieces[0, 2] = lax.ppermute(pieces[0, 1], "y", turn(-1))
    pieces[1, 2] = lax.ppermute(pieces[1, 3], "y", turn(1))
    out = [((f, step, 0), p) for (f, step), p in pieces.items()]
    out += [((f, step, 1), lax.ppermute(p, "c", SWAP)) for (f, step), p in pieces.items()]
    return out


def own_queries_of(sets):
    def kernel(*refs):
        for n in range(4):
            refs[4][32 * n : 32 * n + 32, :] = refs[n][256:288, :]

    return pl.pallas_call(
        kernel,
        out_shape=jax.ShapeDtypeStruct((128, 3 * HEAD), BF),
        compiler_params=room(),
        name="own_queries",
    )(*[in_vmem(a) for a in sets])


def product_to_send(place, critic_in, critic_cot, factor):
    tokens, width = critic_cot.shape

    def kernel(place_ref, in_ref, cot_ref, out_ref):
        out_ref[...] = (
            lax.dot_general(
                in_ref[...], cot_ref[...], (((0,), (0,)), ((), ())), preferred_element_type=F32
            )
            * factor
        ).astype(BF)

    return pl.pallas_call(
        kernel,
        grid_spec=pltpu.PrefetchScalarGridSpec(
            num_scalar_prefetch=1,
            grid=(2,),
            in_specs=[
                pl.BlockSpec((tokens, width // 4), lambda p, place: (0, 2 * (1 - place[2]) + p)),
                pl.BlockSpec((tokens, width), lambda p, place: (0, 0)),
            ],
            out_specs=pl.BlockSpec((width // 4, width), lambda p, place: (p, 0)),
        ),
        out_shape=jax.ShapeDtypeStruct((width // 2, width), BF),
        compiler_params=room(32, dimension_semantics=("arbitrary",)),
        name="product_to_send",
    )(place, in_hbm(critic_in), in_vmem(critic_cot))


def product_and_split(place, critic_in, critic_cot, got, factor):
    tokens, width = critic_cot.shape
    half = width // 2

    def kernel(place_ref, in_ref, cot_ref, got_ref, send_l, send_r, keep_l, keep_r):
        x = place_ref[4]
        p = pl.program_id(0)
        result = lax.dot_general(
            in_ref[...], cot_ref[...], (((0,), (0,)), ((), ())), preferred_element_type=F32
        ) * factor + got_ref[...].astype(F32)
        for u in range(2):
            chunk = 2 * p + u
            left = result[192 * u : 192 * u + 192, :half]
            right = result[192 * u : 192 * u + 192, half:]
            kept_l = (chunk == x) | (chunk == 3 - x)
            kept_r = (chunk == x) | (chunk == (x ^ 1))

            @pl.when(kept_l)
            def _():
                keep_l[jnp.where(chunk == x, 0, 1)] = left

            @pl.when(jnp.logical_not(kept_l))
            def _():
                send_l[jnp.where(chunk == (x ^ 1), 0, 1)] = left.astype(BF)

            @pl.when(kept_r)
            def _():
                keep_r[jnp.where(chunk == x, 0, 1)] = right

            @pl.when(jnp.logical_not(kept_r))
            def _():
                send_r[jnp.where(chunk == 3 - x, 0, 1)] = right.astype(BF)

    whole = pl.BlockSpec((2, 192, half), lambda p, place: (0, 0, 0))
    return pl.pallas_call(
        kernel,
        grid_spec=pltpu.PrefetchScalarGridSpec(
            num_scalar_prefetch=1,
            grid=(2,),
            in_specs=[
                pl.BlockSpec((tokens, width // 4), lambda p, place: (0, 2 * place[2] + p)),
                pl.BlockSpec((tokens, width), lambda p, place: (0, 0)),
                pl.BlockSpec((width // 4, width), lambda p, place: (p, 0)),
            ],
            out_specs=[whole] * 4,
        ),
        out_shape=[jax.ShapeDtypeStruct((2, 192, half), BF)] * 2
        + [jax.ShapeDtypeStruct((2, 192, half), F32)] * 2,
        compiler_params=room(40, dimension_semantics=("arbitrary",)),
        name="product_and_split",
    )(place, in_hbm(critic_in), in_vmem(critic_cot), in_vmem(got))


def onward_of(keep_l, keep_r, got_l, got_r):
    def kernel(kl, kr, gl, gr, out_l, out_r):
        out_l[...] = (kl[0] + gl[1].astype(F32)).astype(BF)
        out_r[...] = (kr[0] + gr[1].astype(F32)).astype(BF)

    _, rows, cols = keep_l.shape
    block = pl.BlockSpec((1, rows, cols), lambda i: (1, 0, 0))
    return pl.pallas_call(
        kernel,
        grid=(1,),
        in_specs=[block] * 2 + [pl.BlockSpec(memory_space=pltpu.VMEM)] * 2,
        out_specs=[pl.BlockSpec((rows, cols), lambda i: (0, 0))] * 2,
        out_shape=[jax.ShapeDtypeStruct((rows, cols), BF)] * 2,
        compiler_params=room(),
        name="onward",
    )(keep_l, keep_r, in_vmem(got_l), in_vmem(got_r))


def cut_along_y(place, keep_l, keep_r, got_l, got_r, last_l, last_r):
    half = keep_l.shape[2]

    def kernel(place_ref, kl, kr, gl, gr, ll, lr, own, one, two, three, total):
        total[:, :half] = kl[0] + gl[0].astype(F32) + ll[...].astype(F32)
        total[:, half:] = kr[0] + gr[0].astype(F32) + lr[...].astype(F32)
        y = place_ref[1]
        for k, ref in enumerate((own, one, two, three)):
            at = ((y + k) % 4) * 24
            for z in range(2):
                rows = total[pl.ds(pl.multiple_of(z * 96 + at, 8), 24), :]
                ref[z] = rows.astype(ref.dtype)

    first = pl.BlockSpec((1, 192, half), lambda i: (0, 0, 0))
    out = pl.BlockSpec((2, 24, 2 * half), lambda i: (0, 0, 0))
    return pl.pallas_call(
        kernel,
        grid=(1,),
        in_specs=[scalars()] + [first] * 2 + [pl.BlockSpec(memory_space=pltpu.VMEM)] * 4,
        out_specs=[out] * 4,
        out_shape=[jax.ShapeDtypeStruct((2, 24, 2 * half), F32)]
        + [jax.ShapeDtypeStruct((2, 24, 2 * half), BF)] * 3,
        scratch_shapes=[pltpu.VMEM((192, 2 * half), F32)],
        compiler_params=room(),
        name="cut_along_y",
    )(place, keep_l, keep_r, *[in_vmem(a) for a in (got_l, got_r, last_l, last_r)])


def cut_to_owners(place, own, others):
    width = own.shape[2]

    def kernel(place_ref, own_ref, a, b, d, *outs):
        total = own_ref[...]
        for ref in (a, b, d):
            total = total + ref[...].astype(F32)
        spot = place_ref[0] * 2 + place_ref[3]
        for here in range(4):

            @pl.when(spot == here)
            def _():
                for n in range(4):
                    z, k = (here ^ n) // 2, (here ^ n) % 2
                    outs[n][...] = total[z, 12 * k : 12 * k + 12, :]

    return pl.pallas_call(
        kernel,
        in_specs=[scalars()] + [pl.BlockSpec()] * 4,
        out_shape=[jax.ShapeDtypeStruct((12, width), F32)] * 4,
        compiler_params=room(),
        name="cut_to_owners",
    )(place, own, *[in_vmem(a) for a in others])


def added(arrays):
    def kernel(*refs):
        refs[-1][...] = (refs[0][...] + refs[1][...]) + (refs[2][...] + refs[3][...])

    return pl.pallas_call(
        kernel,
        out_shape=jax.ShapeDtypeStruct(arrays[0].shape, F32),
        compiler_params=room(),
        name="added",
    )(*[in_vmem(a) for a in arrays])


def weight_gradient(place, critic_in, critic_cot, factor):
    theirs = product_to_send(place, critic_in, critic_cot, factor)
    got = lax.ppermute(theirs, "c", SWAP)
    send_l, send_r, keep_l, keep_r = product_and_split(place, critic_in, critic_cot, got, factor)
    near = [(0, 1), (1, 0), (2, 3), (3, 2)]
    wrap = [(0, 3), (3, 0), (1, 2), (2, 1)]
    got_l = lax.ppermute(send_l, "x", near)
    got_r = lax.ppermute(send_r, "x", wrap)
    on_l, on_r = onward_of(keep_l, keep_r, got_l, got_r)
    last_l = lax.ppermute(on_l, "x", wrap)
    last_r = lax.ppermute(on_r, "x", near)
    own, *others = cut_along_y(place, keep_l, keep_r, got_l, got_r, last_l, last_r)
    others = [lax.ppermute(a, "y", turn(k)) for a, k in zip(others, (1, 2, 3))]
    cuts = cut_to_owners(place, own, others)

    def owner(far_z, far_c):
        spots = [(h, z, k) for h in range(2) for z in range(2) for k in range(2)]
        return [(h * 4 + z * 2 + k, k * 4 + (z ^ far_z) * 2 + (h ^ far_c)) for h, z, k in spots]

    ends = [lax.ppermute(a, ("zh", "zl", "c"), owner(n // 2, n % 2)) for n, a in enumerate(cuts)]
    return added(ends)


def step(
    stream,
    queries,
    new_keys,
    new_values,
    cache_keys,
    cache_values,
    cache_frames,
    group_index,
    timestep,
    gate_table,
    attn_out_weight,
    critic_in,
    critic_cot,
    critic_weight,
):
    zh, x, zl, y, c = (lax.axis_index(a) for a in ("zh", "x", "zl", "y", "c"))
    place = jnp.stack([zl, y, c, zh, x]).astype(jnp.int32)
    near_near, near_far, far_near, far_far = packed(
        place,
        group_index,
        cache_frames,
        (cache_keys[0], new_keys[0], cache_values[0], new_values[0], queries[0]),
    )
    sets = [near_near, lax.ppermute(far_near, "c", SWAP), lax.ppermute(near_far, "zl", SWAP)]
    sets.append(lax.ppermute(lax.ppermute(far_far, "c", SWAP), "zl", SWAP))
    pieces = weight_pieces(critic_weight)

    factor = float(critic_in.shape[0] * 128) ** (-0.5)
    grad_weight = weight_gradient(place, critic_in, critic_cot, factor)

    own = own_queries_of(sets)
    all_queries = [own] + [lax.ppermute(own, "y", turn(k)) for k in (1, 2, 3)]
    partial = attend(sets, all_queries)
    parts = [partial[0]] + [lax.ppermute(partial[k], "y", turn(-k)) for k in (1, 2, 3)]
    mixed = merged(parts)
    cross = [(0, 3), (3, 0), (1, 2), (2, 1)]
    mixed = [
        mixed[0],
        lax.ppermute(mixed[1], "c", SWAP),
        lax.ppermute(mixed[2], "zl", SWAP),
        lax.ppermute(mixed[3], ("zl", "c"), cross),
    ]
    stream_out = streamed(place, timestep, stream[0], gate_table, mixed, attn_out_weight)[None]
    grad_in = grad_of_input(place, critic_cot, pieces)
    return (stream_out, grad_in, grad_weight)


def solution(mesh):
    cut = Mesh(mesh.devices.reshape(2, 4, 2, 4, 2), ("zh", "x", "zl", "y", "c"))
    dp, seq = ("zh", "x"), ("zl", "y", "c")
    whole = dp + seq
    return jax.shard_map(
        step,
        mesh=cut,
        in_specs=(
            P(dp, seq, None),
            P(dp, seq, None),
            P(dp, seq, None),
            P(dp, seq, None),
            P(dp, seq, None),
            P(dp, seq, None),
            P(dp, seq),
            P(dp),
            P(dp),
            P(),
            P(),
            P(whole, None),
            P(whole, None),
            P(whole, None),
        ),
        out_specs=(P(dp, seq, None), P(whole, None), P(whole, None)),
        check_vma=False,
    )
```

```python
import jax
import jax.numpy as jnp
from jax import lax
from jax.experimental import pallas as pl
from jax.experimental.pallas import tpu as pltpu
from jax.sharding import Mesh
from jax.sharding import PartitionSpec as P

HEAD = 128
FRAMES_GROUP = 3
WINDOW_FRAMES = 9
BF = jnp.bfloat16
F32 = jnp.float32


SWAP = [(0, 1), (1, 0)]


def turn(k):
    return [(i, (i + k) % 4) for i in range(4)]


def in_vmem(x):
    return pltpu.with_memory_space_constraint(x, pltpu.VMEM)


def in_hbm(x):
    return pltpu.with_memory_space_constraint(x, pltpu.HBM)


def room(mebibytes=16, **more):
    return pltpu.CompilerParams(vmem_limit_bytes=mebibytes * 2**20, **more)


def any_spec():
    return pl.BlockSpec(memory_space=pl.ANY)


def scalars():
    return pl.BlockSpec(memory_space=pltpu.SMEM)


def packed(place, group_index, frames, arrays):
    width = arrays[0].shape[1]
    quarter = width // 4
    starts, total = [], 0
    for a in arrays:
        starts.append(total)
        total += a.shape[0]

    def kernel(place_ref, group_ref, frames_ref, *refs):
        ins, outs, live_ref = refs[:5], refs[5:9], refs[9]
        first = FRAMES_GROUP * group_ref[0]
        f = frames_ref[...]
        live_ref[...] = jnp.zeros_like(live_ref)
        live_ref[:, 0:128] = jnp.ones((16, 128), F32)
        alive = (f < first) & (f >= first - WINDOW_FRAMES)
        live_ref[:, 0:96] = jnp.broadcast_to(alive.astype(F32), (16, 96))
        spot = place_ref[2] * 2 + place_ref[0]
        for here in range(4):

            @pl.when(spot == here)
            def _():
                for n, q in enumerate((here, here ^ 1, here ^ 2, here ^ 3)):
                    for a, at in zip(ins, starts):
                        outs[n][at : at + a.shape[0], :] = a[:, q * quarter : (q + 1) * quarter]

        for out in outs:
            out[total : total + 16, :] = live_ref[...].astype(BF)

    return pl.pallas_call(
        kernel,
        out_shape=[jax.ShapeDtypeStruct((total + 16, quarter), BF)] * 4,
        in_specs=[scalars(), scalars()] + [pl.BlockSpec()] * 6,
        scratch_shapes=[pltpu.VMEM((16, quarter), F32)],
        compiler_params=room(),
        name="packed",
    )(place, group_index, frames, *[in_hbm(a) for a in arrays])


def attend(sets, queries):
    quarter = 3 * HEAD

    def kernel(*refs):
        set_refs, query_refs, outs = refs[:4], refs[4:8], refs[8:]
        rows = 128
        lane = lax.broadcasted_iota(jnp.int32, (rows, HEAD), 1)
        alive = jnp.concatenate([r[288:304, 0:128] for r in set_refs], axis=1)
        alive = alive.astype(F32)[0:1, :] > 0.5
        stats = [jnp.zeros((rows, HEAD), F32) for _ in range(4)]
        for h in range(3):
            cols = slice(h * HEAD, (h + 1) * HEAD)
            k = jnp.concatenate([r[0:128, cols] for r in set_refs], axis=0)
            v = jnp.concatenate([r[128:256, cols] for r in set_refs], axis=0)
            for r in range(4):
                s = lax.dot_general(
                    query_refs[r][:, cols], k, (((1,), (1,)), ((), ())), preferred_element_type=F32
                ) * (HEAD ** (-0.5))
                s = jnp.where(alive, s, -1e30)
                top = jnp.max(s, axis=1, keepdims=True).astype(BF).astype(F32)
                w = jnp.exp(s - top)
                total = jnp.sum(w, axis=1, keepdims=True)
                o = jnp.dot(w.astype(BF), v, preferred_element_type=F32)
                outs[r][:, cols] = o.astype(BF)
                high = total.astype(BF).astype(F32)
                stats[r] = jnp.where(lane == h, top, stats[r])
                stats[r] = jnp.where(lane == 4 + h, high, stats[r])
                stats[r] = jnp.where(lane == 8 + h, total - high, stats[r])
        for r in range(4):
            outs[r][:, quarter:] = stats[r].astype(BF)

    return pl.pallas_call(
        kernel,
        out_shape=[jax.ShapeDtypeStruct((128, 4 * HEAD), BF)] * 4,
        compiler_params=room(),
        name="attend",
    )(*[in_vmem(a) for a in sets], *[in_vmem(a) for a in queries])


def merged(parts):
    def kernel(*refs):
        ins, outs = refs[:4], refs[4:]
        base = 3 * HEAD
        stats = [r[:, base:].astype(F32) for r in ins]
        for h in range(3):
            tops = [s[:, h : h + 1] for s in stats]
            totals = [s[:, 4 + h : 5 + h] + s[:, 8 + h : 9 + h] for s in stats]
            top = jnp.maximum(jnp.maximum(tops[0], tops[1]), jnp.maximum(tops[2], tops[3]))
            scales = [jnp.exp(t - top) for t in tops]
            total = sum(a * b for a, b in zip(scales, totals))
            cols = slice(h * HEAD, (h + 1) * HEAD)
            summed = sum(r[:, cols].astype(F32) * a for r, a in zip(ins, scales))
            mixed = (summed / total).astype(BF)
            for n in range(4):
                outs[n][:, cols] = mixed[32 * n : 32 * n + 32]

    return pl.pallas_call(
        kernel,
        out_shape=[jax.ShapeDtypeStruct((32, 3 * HEAD), BF)] * 4,
        compiler_params=room(),
        name="merged",
    )(*[in_vmem(a) for a in parts])


def streamed(place, timestep, stream, gate_table, mixed, weight):
    width = weight.shape[1]
    quarter = width // 4

    def kernel(place_ref, step_ref, stream_ref, gate_ref, a_ref, b_ref, c_ref, d_ref, w_ref, out_ref):
        spot = place_ref[2] * 2 + place_ref[0]
        for here in range(4):

            @pl.when(spot == here)
            def _():
                total = jnp.zeros(out_ref.shape, F32)
                for ref, q in zip((a_ref, b_ref, c_ref, d_ref), (here, here ^ 2, here ^ 1, here ^ 3)):
                    total = total + jnp.dot(
                        ref[...], w_ref[q * quarter : (q + 1) * quarter, :], preferred_element_type=F32
                    )
                gate = gate_ref[pl.ds(step_ref[0], 1), :]
                out_ref[...] = (stream_ref[...].astype(F32) + gate * total).astype(BF)

    return pl.pallas_call(
        kernel,
        out_shape=jax.ShapeDtypeStruct(stream.shape, BF),
        in_specs=[scalars(), scalars()] + [pl.BlockSpec()] * 7,
        compiler_params=room(),
        name="streamed",
    )(place, timestep, stream, gate_table, *[in_vmem(a) for a in mixed], weight)


def grad_of_input(place, cot, pieces):
    rows, width = cot.shape
    block = 256
    keys = [k for k, _ in pieces]
    count = len(pieces)

    def kernel(place_ref, cot_ref, *refs):
        ins, (out_ref, buf, weight, sem) = refs[:count], refs[count:]
        zl, y, c, zh, x = (place_ref[n] for n in range(5))

        @pl.when(pl.program_id(0) == 0)
        def _():
            copies = []
            for n, (far, step, other) in enumerate(keys):
                zz = 1 - zl if far else zl
                yy = (y + step) % 4
                cc = 1 - c if other else c
                copies.append(
                    pltpu.make_async_copy(ins[n], buf.at[zz * 8 + yy * 2 + cc], sem.at[n])
                )
                copies[-1].start()
            for copy in copies:
                copy.wait()
            for far in range(2):
                for step in range(4):
                    zz = 1 - zh if far else zh
                    xx = (x + 4 - step) % 4
                    at = 12 * (4 * far + step)
                    for t in range(4):
                        part = [buf[t * 4 + k, at : at + 12, :] for k in range(4)]
                        base = pl.multiple_of(zz * 768 + xx * 192 + t * 48, 16)
                        weight[pl.ds(base, 48), :] = jnp.concatenate(part, axis=0)

        out_ref[...] = lax.dot_general(
            cot_ref[...], weight[...], (((1,), (1,)), ((), ())), preferred_element_type=F32
        ).astype(BF)

    return pl.pallas_call(
        kernel,
        grid=(rows // block,),
        out_shape=jax.ShapeDtypeStruct((rows, width), BF),
        in_specs=[scalars(), pl.BlockSpec((block, width), lambda i: (i, 0))] + [any_spec()] * count,
        out_specs=pl.BlockSpec((block, width), lambda i: (i, 0)),
        scratch_shapes=[
            pltpu.VMEM((16, 96, width), BF),
            pltpu.VMEM((width, width), BF),
            pltpu.SemaphoreType.DMA((count,)),
        ],
        compiler_params=room(28, dimension_semantics=("arbitrary",)),
        name="grad_of_input",
    )(place, cot, *[in_vmem(p) for _, p in pieces])


def joined(arrays, first_in_vmem=False):
    rows = [a.shape[0] for a in arrays]

    def kernel(*refs):
        out_ref, at = refs[-1], 0
        for ref, n in zip(refs[:-1], rows):
            out_ref[at : at + n, :] = ref[...]
            at += n

    place_first = in_vmem if first_in_vmem else in_hbm
    return pl.pallas_call(
        kernel,
        out_shape=pltpu.VMEM((sum(rows), arrays[0].shape[1]), arrays[0].dtype),
        compiler_params=room(),
        name="joined",
    )(place_first(arrays[0]), *[in_vmem(a) for a in arrays[1:]])


def weight_pieces(weight):
    on_x = [weight] + [lax.ppermute(weight, "x", turn(k)) for k in (1, 2, 3)]
    on_x = joined(on_x)
    far = lax.ppermute(on_x, "zh", SWAP)
    near = joined([on_x, far], True)
    far = lax.ppermute(near, "zl", SWAP)
    pieces = {(0, 0): near, (1, 0): far}
    for f in range(2):
        pieces[f, 3] = lax.ppermute(pieces[f, 0], "y", turn(1))
        pieces[f, 1] = lax.ppermute(pieces[f, 0], "y", turn(-1))
    pieces[0, 2] = lax.ppermute(pieces[0, 1], "y", turn(-1))
    pieces[1, 2] = lax.ppermute(pieces[1, 3], "y", turn(1))
    out = [((f, step, 0), p) for (f, step), p in pieces.items()]
    out += [((f, step, 1), lax.ppermute(p, "c", SWAP)) for (f, step), p in pieces.items()]
    return out


def own_queries_of(sets):
    def kernel(*refs):
        for n in range(4):
            refs[4][32 * n : 32 * n + 32, :] = refs[n][256:288, :]

    return pl.pallas_call(
        kernel,
        out_shape=pltpu.VMEM((128, 3 * HEAD), BF),
        compiler_params=room(),
        name="own_queries",
    )(*[in_vmem(a) for a in sets])


def product_to_send(place, critic_in, critic_cot, factor):
    tokens, width = critic_cot.shape

    def kernel(place_ref, in_ref, cot_ref, out_ref):
        out_ref[...] = (
            lax.dot_general(
                in_ref[...], cot_ref[...], (((0,), (0,)), ((), ())), preferred_element_type=F32
            )
            * factor
        ).astype(BF)

    return pl.pallas_call(
        kernel,
        grid_spec=pltpu.PrefetchScalarGridSpec(
            num_scalar_prefetch=1,
            grid=(4,),
            in_specs=[
                pl.BlockSpec((tokens, width // 2), lambda p, place: (0, 1 - place[2])),
                pl.BlockSpec((tokens, width // 4), lambda p, place: (0, p)),
            ],
            out_specs=pl.BlockSpec((width // 2, width // 4), lambda p, place: (0, p)),
        ),
        out_shape=jax.ShapeDtypeStruct((width // 2, width), BF),
        compiler_params=room(32, dimension_semantics=("arbitrary",)),
        name="product_to_send",
    )(place, in_hbm(critic_in), in_vmem(critic_cot))


def product_and_split(place, critic_in, critic_cot, got, factor):
    tokens, width = critic_cot.shape
    half = width // 2

    def kernel(place_ref, in_ref, cot_ref, got_ref, send_l, send_r, keep_l, keep_r):
        x = place_ref[4]
        p = pl.program_id(0)
        result = lax.dot_general(
            in_ref[...], cot_ref[...], (((0,), (0,)), ((), ())), preferred_element_type=F32
        ) * factor + got_ref[...].astype(F32)
        for u in range(2):
            chunk = 2 * p + u
            left = result[192 * u : 192 * u + 192, :half]
            right = result[192 * u : 192 * u + 192, half:]
            kept_l = (chunk == x) | (chunk == 3 - x)
            kept_r = (chunk == x) | (chunk == (x ^ 1))

            @pl.when(kept_l)
            def _():
                keep_l[jnp.where(chunk == x, 0, 1)] = left

            @pl.when(jnp.logical_not(kept_l))
            def _():
                send_l[jnp.where(chunk == (x ^ 1), 0, 1)] = left.astype(BF)

            @pl.when(kept_r)
            def _():
                keep_r[jnp.where(chunk == x, 0, 1)] = right

            @pl.when(jnp.logical_not(kept_r))
            def _():
                send_r[jnp.where(chunk == 3 - x, 0, 1)] = right.astype(BF)

    whole = pl.BlockSpec((2, 192, half), lambda p, place: (0, 0, 0))
    return pl.pallas_call(
        kernel,
        grid_spec=pltpu.PrefetchScalarGridSpec(
            num_scalar_prefetch=1,
            grid=(2,),
            in_specs=[
                pl.BlockSpec((tokens, width // 4), lambda p, place: (0, 2 * place[2] + p)),
                pl.BlockSpec((tokens, width), lambda p, place: (0, 0)),
                pl.BlockSpec((width // 4, width), lambda p, place: (p, 0)),
            ],
            out_specs=[whole] * 4,
        ),
        out_shape=[jax.ShapeDtypeStruct((2, 192, half), BF)] * 2
        + [jax.ShapeDtypeStruct((2, 192, half), F32)] * 2,
        compiler_params=room(40, dimension_semantics=("arbitrary",)),
        name="product_and_split",
    )(place, in_hbm(critic_in), in_vmem(critic_cot), in_vmem(got))


def onward_of(keep_l, keep_r, got_l, got_r):
    def kernel(kl, kr, gl, gr, out_l, out_r):
        out_l[...] = (kl[0] + gl[1].astype(F32)).astype(BF)
        out_r[...] = (kr[0] + gr[1].astype(F32)).astype(BF)

    _, rows, cols = keep_l.shape
    block = pl.BlockSpec((1, rows, cols), lambda i: (1, 0, 0))
    return pl.pallas_call(
        kernel,
        grid=(1,),
        in_specs=[block] * 2 + [pl.BlockSpec(memory_space=pltpu.VMEM)] * 2,
        out_specs=[pl.BlockSpec((rows, cols), lambda i: (0, 0))] * 2,
        out_shape=[jax.ShapeDtypeStruct((rows, cols), BF)] * 2,
        compiler_params=room(),
        name="onward",
    )(keep_l, keep_r, in_vmem(got_l), in_vmem(got_r))


def cut_along_y(place, keep_l, keep_r, got_l, got_r, last_l, last_r):
    half = keep_l.shape[2]

    def kernel(place_ref, kl, kr, gl, gr, ll, lr, own, one, two, three, total):
        total[:, :half] = kl[0] + gl[0].astype(F32) + ll[...].astype(F32)
        total[:, half:] = kr[0] + gr[0].astype(F32) + lr[...].astype(F32)
        y = place_ref[1]
        for k, ref in enumerate((own, one, two, three)):
            at = ((y + k) % 4) * 24
            for z in range(2):
                rows = total[pl.ds(pl.multiple_of(z * 96 + at, 8), 24), :]
                ref[z] = rows.astype(ref.dtype)

    first = pl.BlockSpec((1, 192, half), lambda i: (0, 0, 0))
    out = pl.BlockSpec((2, 24, 2 * half), lambda i: (0, 0, 0))
    return pl.pallas_call(
        kernel,
        grid=(1,),
        in_specs=[scalars()] + [first] * 2 + [pl.BlockSpec(memory_space=pltpu.VMEM)] * 4,
        out_specs=[out] * 4,
        out_shape=[jax.ShapeDtypeStruct((2, 24, 2 * half), F32)]
        + [jax.ShapeDtypeStruct((2, 24, 2 * half), BF)] * 3,
        scratch_shapes=[pltpu.VMEM((192, 2 * half), F32)],
        compiler_params=room(),
        name="cut_along_y",
    )(place, keep_l, keep_r, *[in_vmem(a) for a in (got_l, got_r, last_l, last_r)])


def cut_to_owners(place, own, others):
    width = own.shape[2]

    def kernel(place_ref, own_ref, a, b, d, *outs):
        total = own_ref[...]
        for ref in (a, b, d):
            total = total + ref[...].astype(F32)
        spot = place_ref[0] * 2 + place_ref[3]
        for here in range(4):

            @pl.when(spot == here)
            def _():
                for n in range(4):
                    z, k = (here ^ n) // 2, (here ^ n) % 2
                    outs[n][...] = total[z, 12 * k : 12 * k + 12, :]

    return pl.pallas_call(
        kernel,
        in_specs=[scalars()] + [pl.BlockSpec()] * 4,
        out_shape=[jax.ShapeDtypeStruct((12, width), F32)] * 4,
        compiler_params=room(),
        name="cut_to_owners",
    )(place, own, *[in_vmem(a) for a in others])


def added(arrays):
    def kernel(*refs):
        refs[-1][...] = (refs[0][...] + refs[1][...]) + (refs[2][...] + refs[3][...])

    return pl.pallas_call(
        kernel,
        out_shape=jax.ShapeDtypeStruct(arrays[0].shape, F32),
        compiler_params=room(),
        name="added",
    )(*[in_vmem(a) for a in arrays])


def weight_gradient(place, critic_in, critic_cot, factor):
    theirs = product_to_send(place, critic_in, critic_cot, factor)
    got = lax.ppermute(theirs, "c", SWAP)
    send_l, send_r, keep_l, keep_r = product_and_split(place, critic_in, critic_cot, got, factor)
    near = [(0, 1), (1, 0), (2, 3), (3, 2)]
    wrap = [(0, 3), (3, 0), (1, 2), (2, 1)]
    got_l = lax.ppermute(send_l, "x", near)
    got_r = lax.ppermute(send_r, "x", wrap)
    on_l, on_r = onward_of(keep_l, keep_r, got_l, got_r)
    last_l = lax.ppermute(on_l, "x", wrap)
    last_r = lax.ppermute(on_r, "x", near)
    own, *others = cut_along_y(place, keep_l, keep_r, got_l, got_r, last_l, last_r)
    others = [lax.ppermute(a, "y", turn(k)) for a, k in zip(others, (1, 2, 3))]
    cuts = cut_to_owners(place, own, others)

    def owner(far_z, far_c):
        spots = [(h, z, k) for h in range(2) for z in range(2) for k in range(2)]
        return [(h * 4 + z * 2 + k, k * 4 + (z ^ far_z) * 2 + (h ^ far_c)) for h, z, k in spots]

    ends = [lax.ppermute(a, ("zh", "zl", "c"), owner(n // 2, n % 2)) for n, a in enumerate(cuts)]
    return added(ends)


def step(
    stream,
    queries,
    new_keys,
    new_values,
    cache_keys,
    cache_values,
    cache_frames,
    group_index,
    timestep,
    gate_table,
    attn_out_weight,
    critic_in,
    critic_cot,
    critic_weight,
):
    zh, x, zl, y, c = (lax.axis_index(a) for a in ("zh", "x", "zl", "y", "c"))
    place = jnp.stack([zl, y, c, zh, x]).astype(jnp.int32)
    near_near, near_far, far_near, far_far = packed(
        place,
        group_index,
        cache_frames,
        (cache_keys[0], new_keys[0], cache_values[0], new_values[0], queries[0]),
    )
    sets = [near_near, lax.ppermute(far_near, "c", SWAP), lax.ppermute(near_far, "zl", SWAP)]
    sets.append(lax.ppermute(lax.ppermute(far_far, "c", SWAP), "zl", SWAP))
    pieces = weight_pieces(critic_weight)

    factor = float(critic_in.shape[0] * 128) ** (-0.5)
    grad_weight = weight_gradient(place, critic_in, critic_cot, factor)

    own = own_queries_of(sets)
    all_queries = [own] + [lax.ppermute(own, "y", turn(k)) for k in (1, 2, 3)]
    partial = attend(sets, all_queries)
    parts = [partial[0]] + [lax.ppermute(partial[k], "y", turn(-k)) for k in (1, 2, 3)]
    mixed = merged(parts)
    cross = [(0, 3), (3, 0), (1, 2), (2, 1)]
    mixed = [
        mixed[0],
        lax.ppermute(mixed[1], "c", SWAP),
        lax.ppermute(mixed[2], "zl", SWAP),
        lax.ppermute(mixed[3], ("zl", "c"), cross),
    ]
    stream_out = streamed(place, timestep, stream[0], gate_table, mixed, attn_out_weight)[None]
    grad_in = grad_of_input(place, critic_cot, pieces)
    return (stream_out, grad_in, grad_weight)


def solution(mesh):
    cut = Mesh(mesh.devices.reshape(2, 4, 2, 4, 2), ("zh", "x", "zl", "y", "c"))
    dp, seq = ("zh", "x"), ("zl", "y", "c")
    whole = dp + seq
    return jax.shard_map(
        step,
        mesh=cut,
        in_specs=(
            P(dp, seq, None),
            P(dp, seq, None),
            P(dp, seq, None),
            P(dp, seq, None),
            P(dp, seq, None),
            P(dp, seq, None),
            P(dp, seq),
            P(dp),
            P(dp),
            P(),
            P(),
            P(whole, None),
            P(whole, None),
            P(whole, None),
        ),
        out_specs=(P(dp, seq, None), P(whole, None), P(whole, None)),
        check_vma=False,
    )
```

```python
import jax
import jax.numpy as jnp
from jax import lax
from jax.experimental import pallas as pl
from jax.experimental.pallas import tpu as pltpu
from jax.sharding import Mesh
from jax.sharding import PartitionSpec as P

HEAD = 128
FRAMES_GROUP = 3
WINDOW_FRAMES = 9
BF = jnp.bfloat16
F32 = jnp.float32


SWAP = [(0, 1), (1, 0)]


def turn(k):
    return [(i, (i + k) % 4) for i in range(4)]


def in_vmem(x):
    return pltpu.with_memory_space_constraint(x, pltpu.VMEM)


def in_hbm(x):
    return pltpu.with_memory_space_constraint(x, pltpu.HBM)


def room(mebibytes=16, **more):
    return pltpu.CompilerParams(vmem_limit_bytes=mebibytes * 2**20, **more)


def any_spec():
    return pl.BlockSpec(memory_space=pl.ANY)


def scalars():
    return pl.BlockSpec(memory_space=pltpu.SMEM)


def packed(place, group_index, frames, arrays):
    width = arrays[0].shape[1]
    quarter = width // 4
    starts, total = [], 0
    for a in arrays:
        starts.append(total)
        total += a.shape[0]

    def kernel(place_ref, group_ref, frames_ref, *refs):
        ins, outs, live_ref = refs[:5], refs[5:9], refs[9]
        first = FRAMES_GROUP * group_ref[0]
        f = frames_ref[...]
        live_ref[...] = jnp.zeros_like(live_ref)
        live_ref[:, 0:128] = jnp.ones((16, 128), F32)
        alive = (f < first) & (f >= first - WINDOW_FRAMES)
        live_ref[:, 0:96] = jnp.broadcast_to(alive.astype(F32), (16, 96))
        spot = place_ref[2] * 2 + place_ref[0]
        for here in range(4):

            @pl.when(spot == here)
            def _():
                for n, q in enumerate((here, here ^ 1, here ^ 2, here ^ 3)):
                    for a, at in zip(ins, starts):
                        outs[n][at : at + a.shape[0], :] = a[:, q * quarter : (q + 1) * quarter]

        for out in outs:
            out[total : total + 16, :] = live_ref[...].astype(BF)

    return pl.pallas_call(
        kernel,
        out_shape=[jax.ShapeDtypeStruct((total + 16, quarter), BF)] * 4,
        in_specs=[scalars(), scalars()] + [pl.BlockSpec()] * 6,
        scratch_shapes=[pltpu.VMEM((16, quarter), F32)],
        compiler_params=room(),
        name="packed",
    )(place, group_index, frames, *[in_hbm(a) for a in arrays])


def attend(sets, queries):
    quarter = 3 * HEAD

    def kernel(*refs):
        set_refs, query_refs, outs = refs[:4], refs[4:8], refs[8:]
        rows = 128
        lane = lax.broadcasted_iota(jnp.int32, (rows, HEAD), 1)
        alive = jnp.concatenate([r[288:304, 0:128] for r in set_refs], axis=1)
        alive = alive.astype(F32)[0:1, :] > 0.5
        stats = [jnp.zeros((rows, HEAD), F32) for _ in range(4)]
        for h in range(3):
            cols = slice(h * HEAD, (h + 1) * HEAD)
            k = jnp.concatenate([r[0:128, cols] for r in set_refs], axis=0)
            v = jnp.concatenate([r[128:256, cols] for r in set_refs], axis=0)
            for r in range(4):
                s = lax.dot_general(
                    query_refs[r][:, cols], k, (((1,), (1,)), ((), ())), preferred_element_type=F32
                ) * (HEAD ** (-0.5))
                s = jnp.where(alive, s, -1e30)
                top = jnp.max(s, axis=1, keepdims=True).astype(BF).astype(F32)
                w = jnp.exp(s - top)
                total = jnp.sum(w, axis=1, keepdims=True)
                o = jnp.dot(w.astype(BF), v, preferred_element_type=F32)
                outs[r][:, cols] = o.astype(BF)
                high = total.astype(BF).astype(F32)
                stats[r] = jnp.where(lane == h, top, stats[r])
                stats[r] = jnp.where(lane == 4 + h, high, stats[r])
                stats[r] = jnp.where(lane == 8 + h, total - high, stats[r])
        for r in range(4):
            outs[r][:, quarter:] = stats[r].astype(BF)

    return pl.pallas_call(
        kernel,
        out_shape=[jax.ShapeDtypeStruct((128, 4 * HEAD), BF)] * 4,
        compiler_params=room(),
        name="attend",
    )(*[in_vmem(a) for a in sets], *[in_vmem(a) for a in queries])


def merged(parts):
    def kernel(*refs):
        ins, outs = refs[:4], refs[4:]
        base = 3 * HEAD
        stats = [r[:, base:].astype(F32) for r in ins]
        for h in range(3):
            tops = [s[:, h : h + 1] for s in stats]
            totals = [s[:, 4 + h : 5 + h] + s[:, 8 + h : 9 + h] for s in stats]
            top = jnp.maximum(jnp.maximum(tops[0], tops[1]), jnp.maximum(tops[2], tops[3]))
            scales = [jnp.exp(t - top) for t in tops]
            total = sum(a * b for a, b in zip(scales, totals))
            cols = slice(h * HEAD, (h + 1) * HEAD)
            summed = sum(r[:, cols].astype(F32) * a for r, a in zip(ins, scales))
            mixed = (summed / total).astype(BF)
            for n in range(4):
                outs[n][:, cols] = mixed[32 * n : 32 * n + 32]

    return pl.pallas_call(
        kernel,
        out_shape=[jax.ShapeDtypeStruct((32, 3 * HEAD), BF)] * 4,
        compiler_params=room(),
        name="merged",
    )(*[in_vmem(a) for a in parts])


def streamed(place, timestep, stream, gate_table, mixed, weight):
    width = weight.shape[1]
    quarter = width // 4

    def kernel(place_ref, step_ref, stream_ref, gate_ref, a_ref, b_ref, c_ref, d_ref, w_ref, out_ref):
        spot = place_ref[2] * 2 + place_ref[0]
        for here in range(4):

            @pl.when(spot == here)
            def _():
                total = jnp.zeros(out_ref.shape, F32)
                for ref, q in zip((a_ref, b_ref, c_ref, d_ref), (here, here ^ 2, here ^ 1, here ^ 3)):
                    total = total + jnp.dot(
                        ref[...], w_ref[q * quarter : (q + 1) * quarter, :], preferred_element_type=F32
                    )
                gate = gate_ref[pl.ds(step_ref[0], 1), :]
                out_ref[...] = (stream_ref[...].astype(F32) + gate * total).astype(BF)

    return pl.pallas_call(
        kernel,
        out_shape=jax.ShapeDtypeStruct(stream.shape, BF),
        in_specs=[scalars(), scalars()] + [pl.BlockSpec()] * 7,
        compiler_params=room(),
        name="streamed",
    )(place, timestep, stream, gate_table, *[in_vmem(a) for a in mixed], weight)


def grad_of_input(place, cot, pieces):
    rows, width = cot.shape
    block = 256
    keys = [k for k, _ in pieces]
    count = len(pieces)

    def kernel(place_ref, cot_ref, *refs):
        ins, (out_ref, buf, weight, sem) = refs[:count], refs[count:]
        zl, y, c, zh, x = (place_ref[n] for n in range(5))

        @pl.when(pl.program_id(0) == 0)
        def _():
            copies = []
            for n, (far, step, other) in enumerate(keys):
                zz = 1 - zl if far else zl
                yy = (y + step) % 4
                cc = 1 - c if other else c
                copies.append(
                    pltpu.make_async_copy(ins[n], buf.at[zz * 8 + yy * 2 + cc], sem.at[n])
                )
                copies[-1].start()
            for copy in copies:
                copy.wait()
            for far in range(2):
                for step in range(4):
                    zz = 1 - zh if far else zh
                    xx = (x + 4 - step) % 4
                    at = 12 * (4 * far + step)
                    for t in range(4):
                        part = [buf[t * 4 + k, at : at + 12, :] for k in range(4)]
                        base = pl.multiple_of(zz * 768 + xx * 192 + t * 48, 16)
                        weight[pl.ds(base, 48), :] = jnp.concatenate(part, axis=0)

        out_ref[...] = lax.dot_general(
            cot_ref[...], weight[...], (((1,), (1,)), ((), ())), preferred_element_type=F32
        ).astype(BF)

    return pl.pallas_call(
        kernel,
        grid=(rows // block,),
        out_shape=jax.ShapeDtypeStruct((rows, width), BF),
        in_specs=[scalars(), pl.BlockSpec((block, width), lambda i: (i, 0))] + [any_spec()] * count,
        out_specs=pl.BlockSpec((block, width), lambda i: (i, 0)),
        scratch_shapes=[
            pltpu.VMEM((16, 96, width), BF),
            pltpu.VMEM((width, width), BF),
            pltpu.SemaphoreType.DMA((count,)),
        ],
        compiler_params=room(28, dimension_semantics=("arbitrary",)),
        name="grad_of_input",
    )(place, cot, *[in_vmem(p) for _, p in pieces])


def joined(arrays, first_in_vmem=False):
    rows = [a.shape[0] for a in arrays]

    def kernel(*refs):
        out_ref, at = refs[-1], 0
        for ref, n in zip(refs[:-1], rows):
            out_ref[at : at + n, :] = ref[...]
            at += n

    place_first = in_vmem if first_in_vmem else in_hbm
    return pl.pallas_call(
        kernel,
        out_shape=pltpu.VMEM((sum(rows), arrays[0].shape[1]), arrays[0].dtype),
        compiler_params=room(),
        name="joined",
    )(place_first(arrays[0]), *[in_vmem(a) for a in arrays[1:]])


def weight_pieces(weight):
    on_x = [weight] + [lax.ppermute(weight, "x", turn(k)) for k in (1, 2, 3)]
    on_x = joined(on_x)
    far = lax.ppermute(on_x, "zh", SWAP)
    near = joined([on_x, far], True)
    far = lax.ppermute(near, "zl", SWAP)
    pieces = {(0, 0): near, (1, 0): far}
    for f in range(2):
        pieces[f, 3] = lax.ppermute(pieces[f, 0], "y", turn(1))
        pieces[f, 1] = lax.ppermute(pieces[f, 0], "y", turn(-1))
    pieces[0, 2] = lax.ppermute(pieces[0, 1], "y", turn(-1))
    pieces[1, 2] = lax.ppermute(pieces[1, 3], "y", turn(1))
    out = [((f, step, 0), p) for (f, step), p in pieces.items()]
    out += [((f, step, 1), lax.ppermute(p, "c", SWAP)) for (f, step), p in pieces.items()]
    return out


def own_queries_of(sets):
    def kernel(*refs):
        for n in range(4):
            refs[4][32 * n : 32 * n + 32, :] = refs[n][256:288, :]

    return pl.pallas_call(
        kernel,
        out_shape=pltpu.VMEM((128, 3 * HEAD), BF),
        compiler_params=room(),
        name="own_queries",
    )(*[in_vmem(a) for a in sets])


def product_to_send(place, critic_in, critic_cot, factor):
    tokens, width = critic_cot.shape

    def kernel(place_ref, in_ref, cot_ref, out_ref):
        out_ref[...] = (
            lax.dot_general(
                in_ref[...], cot_ref[...], (((0,), (0,)), ((), ())), preferred_element_type=F32
            )
            * factor
        ).astype(BF)

    return pl.pallas_call(
        kernel,
        grid_spec=pltpu.PrefetchScalarGridSpec(
            num_scalar_prefetch=1,
            grid=(2,),
            in_specs=[
                pl.BlockSpec((tokens, width // 4), lambda p, place: (0, 2 * (1 - place[2]) + p)),
                pl.BlockSpec((tokens, width), lambda p, place: (0, 0)),
            ],
            out_specs=pl.BlockSpec((width // 4, width), lambda p, place: (p, 0)),
        ),
        out_shape=jax.ShapeDtypeStruct((width // 2, width), BF),
        compiler_params=room(32, dimension_semantics=("arbitrary",)),
        name="product_to_send",
    )(place, in_hbm(critic_in), in_vmem(critic_cot))


def product_and_split(place, critic_in, critic_cot, got, factor):
    tokens, width = critic_cot.shape
    half = width // 2

    def kernel(place_ref, in_ref, cot_ref, got_ref, send_l, send_r, keep_l, keep_r):
        x = place_ref[4]
        p = pl.program_id(0)
        result = lax.dot_general(
            in_ref[...], cot_ref[...], (((0,), (0,)), ((), ())), preferred_element_type=F32
        ) * factor + got_ref[...].astype(F32)
        for u in range(2):
            chunk = 2 * p + u
            left = result[192 * u : 192 * u + 192, :half]
            right = result[192 * u : 192 * u + 192, half:]
            kept_l = (chunk == x) | (chunk == 3 - x)
            kept_r = (chunk == x) | (chunk == (x ^ 1))

            @pl.when(kept_l)
            def _():
                keep_l[jnp.where(chunk == x, 0, 1)] = left

            @pl.when(jnp.logical_not(kept_l))
            def _():
                send_l[jnp.where(chunk == (x ^ 1), 0, 1)] = left.astype(BF)

            @pl.when(kept_r)
            def _():
                keep_r[jnp.where(chunk == x, 0, 1)] = right

            @pl.when(jnp.logical_not(kept_r))
            def _():
                send_r[jnp.where(chunk == 3 - x, 0, 1)] = right.astype(BF)

    whole = pl.BlockSpec((2, 192, half), lambda p, place: (0, 0, 0))
    return pl.pallas_call(
        kernel,
        grid_spec=pltpu.PrefetchScalarGridSpec(
            num_scalar_prefetch=1,
            grid=(2,),
            in_specs=[
                pl.BlockSpec((tokens, width // 4), lambda p, place: (0, 2 * place[2] + p)),
                pl.BlockSpec((tokens, width), lambda p, place: (0, 0)),
                pl.BlockSpec((width // 4, width), lambda p, place: (p, 0)),
            ],
            out_specs=[whole] * 4,
        ),
        out_shape=[jax.ShapeDtypeStruct((2, 192, half), BF)] * 2
        + [jax.ShapeDtypeStruct((2, 192, half), F32)] * 2,
        compiler_params=room(40, dimension_semantics=("arbitrary",)),
        name="product_and_split",
    )(place, in_hbm(critic_in), in_vmem(critic_cot), in_vmem(got))


def onward_of(keep_l, keep_r, got_l, got_r):
    def kernel(kl, kr, gl, gr, out_l, out_r):
        out_l[...] = (kl[0] + gl[1].astype(F32)).astype(BF)
        out_r[...] = (kr[0] + gr[1].astype(F32)).astype(BF)

    _, rows, cols = keep_l.shape
    block = pl.BlockSpec((1, rows, cols), lambda i: (1, 0, 0))
    return pl.pallas_call(
        kernel,
        grid=(1,),
        in_specs=[block] * 2 + [pl.BlockSpec(memory_space=pltpu.VMEM)] * 2,
        out_specs=[pl.BlockSpec((rows, cols), lambda i: (0, 0))] * 2,
        out_shape=[jax.ShapeDtypeStruct((rows, cols), BF)] * 2,
        compiler_params=room(),
        name="onward",
    )(keep_l, keep_r, in_vmem(got_l), in_vmem(got_r))


def cut_along_y(place, keep_l, keep_r, got_l, got_r, last_l, last_r):
    half = keep_l.shape[2]

    def kernel(place_ref, kl, kr, gl, gr, ll, lr, own, one, two, three, total):
        total[:, :half] = kl[0] + gl[0].astype(F32) + ll[...].astype(F32)
        total[:, half:] = kr[0] + gr[0].astype(F32) + lr[...].astype(F32)
        y = place_ref[1]
        for k, ref in enumerate((own, one, two, three)):
            at = ((y + k) % 4) * 24
            for z in range(2):
                rows = total[pl.ds(pl.multiple_of(z * 96 + at, 8), 24), :]
                ref[z] = rows.astype(ref.dtype)

    first = pl.BlockSpec((1, 192, half), lambda i: (0, 0, 0))
    out = pl.BlockSpec((2, 24, 2 * half), lambda i: (0, 0, 0))
    return pl.pallas_call(
        kernel,
        grid=(1,),
        in_specs=[scalars()] + [first] * 2 + [pl.BlockSpec(memory_space=pltpu.VMEM)] * 4,
        out_specs=[out] * 4,
        out_shape=[jax.ShapeDtypeStruct((2, 24, 2 * half), F32)]
        + [jax.ShapeDtypeStruct((2, 24, 2 * half), BF)] * 3,
        scratch_shapes=[pltpu.VMEM((192, 2 * half), F32)],
        compiler_params=room(),
        name="cut_along_y",
    )(place, keep_l, keep_r, *[in_vmem(a) for a in (got_l, got_r, last_l, last_r)])


def cut_to_owners(place, own, others):
    width = own.shape[2]

    def kernel(place_ref, own_ref, a, b, d, *outs):
        total = own_ref[...]
        for ref in (a, b, d):
            total = total + ref[...].astype(F32)
        spot = place_ref[0] * 2 + place_ref[3]
        for here in range(4):

            @pl.when(spot == here)
            def _():
                for n in range(4):
                    z, k = (here ^ n) // 2, (here ^ n) % 2
                    outs[n][...] = total[z, 12 * k : 12 * k + 12, :]

    return pl.pallas_call(
        kernel,
        in_specs=[scalars()] + [pl.BlockSpec()] * 4,
        out_shape=[jax.ShapeDtypeStruct((12, width), F32)] * 4,
        compiler_params=room(),
        name="cut_to_owners",
    )(place, own, *[in_vmem(a) for a in others])


def added(arrays):
    def kernel(*refs):
        refs[-1][...] = (refs[0][...] + refs[1][...]) + (refs[2][...] + refs[3][...])

    return pl.pallas_call(
        kernel,
        out_shape=jax.ShapeDtypeStruct(arrays[0].shape, F32),
        compiler_params=room(),
        name="added",
    )(*[in_vmem(a) for a in arrays])


def weight_gradient(place, critic_in, critic_cot, factor):
    theirs = product_to_send(place, critic_in, critic_cot, factor)
    got = lax.ppermute(theirs, "c", SWAP)
    send_l, send_r, keep_l, keep_r = product_and_split(place, critic_in, critic_cot, got, factor)
    near = [(0, 1), (1, 0), (2, 3), (3, 2)]
    wrap = [(0, 3), (3, 0), (1, 2), (2, 1)]
    got_l = lax.ppermute(send_l, "x", near)
    got_r = lax.ppermute(send_r, "x", wrap)
    on_l, on_r = onward_of(keep_l, keep_r, got_l, got_r)
    last_l = lax.ppermute(on_l, "x", wrap)
    last_r = lax.ppermute(on_r, "x", near)
    own, *others = cut_along_y(place, keep_l, keep_r, got_l, got_r, last_l, last_r)
    others = [lax.ppermute(a, "y", turn(k)) for a, k in zip(others, (1, 2, 3))]
    cuts = cut_to_owners(place, own, others)

    def owner(far_z, far_c):
        spots = [(h, z, k) for h in range(2) for z in range(2) for k in range(2)]
        return [(h * 4 + z * 2 + k, k * 4 + (z ^ far_z) * 2 + (h ^ far_c)) for h, z, k in spots]

    ends = [lax.ppermute(a, ("zh", "zl", "c"), owner(n // 2, n % 2)) for n, a in enumerate(cuts)]
    return added(ends)


def step(
    stream,
    queries,
    new_keys,
    new_values,
    cache_keys,
    cache_values,
    cache_frames,
    group_index,
    timestep,
    gate_table,
    attn_out_weight,
    critic_in,
    critic_cot,
    critic_weight,
):
    zh, x, zl, y, c = (lax.axis_index(a) for a in ("zh", "x", "zl", "y", "c"))
    place = jnp.stack([zl, y, c, zh, x]).astype(jnp.int32)
    near_near, near_far, far_near, far_far = packed(
        place,
        group_index,
        cache_frames,
        (cache_keys[0], new_keys[0], cache_values[0], new_values[0], queries[0]),
    )
    sets = [near_near, lax.ppermute(far_near, "c", SWAP), lax.ppermute(near_far, "zl", SWAP)]
    sets.append(lax.ppermute(lax.ppermute(far_far, "c", SWAP), "zl", SWAP))
    pieces = weight_pieces(critic_weight)

    factor = float(critic_in.shape[0] * 128) ** (-0.5)
    grad_weight = weight_gradient(place, critic_in, critic_cot, factor)

    own = own_queries_of(sets)
    all_queries = [own] + [lax.ppermute(own, "y", turn(k)) for k in (1, 2, 3)]
    partial = attend(sets, all_queries)
    parts = [partial[0]] + [lax.ppermute(partial[k], "y", turn(-k)) for k in (1, 2, 3)]
    mixed = merged(parts)
    cross = [(0, 3), (3, 0), (1, 2), (2, 1)]
    mixed = [
        mixed[0],
        lax.ppermute(mixed[1], "c", SWAP),
        lax.ppermute(mixed[2], "zl", SWAP),
        lax.ppermute(mixed[3], ("zl", "c"), cross),
    ]
    stream_out = streamed(place, timestep, stream[0], gate_table, mixed, attn_out_weight)[None]
    grad_in = grad_of_input(place, critic_cot, pieces)
    return (stream_out, grad_in, grad_weight)


def solution(mesh):
    cut = Mesh(mesh.devices.reshape(2, 4, 2, 4, 2), ("zh", "x", "zl", "y", "c"))
    dp, seq = ("zh", "x"), ("zl", "y", "c")
    whole = dp + seq
    return jax.shard_map(
        step,
        mesh=cut,
        in_specs=(
            P(dp, seq, None),
            P(dp, seq, None),
            P(dp, seq, None),
            P(dp, seq, None),
            P(dp, seq, None),
            P(dp, seq, None),
            P(dp, seq),
            P(dp),
            P(dp),
            P(),
            P(),
            P(whole, None),
            P(whole, None),
            P(whole, None),
        ),
        out_specs=(P(dp, seq, None), P(whole, None), P(whole, None)),
        check_vma=False,
    )
```

```python
import jax
import jax.numpy as jnp
from jax import lax
from jax.experimental import pallas as pl
from jax.experimental.pallas import tpu as pltpu
from jax.sharding import Mesh
from jax.sharding import PartitionSpec as P

HEAD = 128
FRAMES_GROUP = 3
WINDOW_FRAMES = 9
BF = jnp.bfloat16
F32 = jnp.float32


SWAP = [(0, 1), (1, 0)]


def turn(k):
    return [(i, (i + k) % 4) for i in range(4)]


def in_vmem(x):
    return pltpu.with_memory_space_constraint(x, pltpu.VMEM)


def in_hbm(x):
    return pltpu.with_memory_space_constraint(x, pltpu.HBM)


def room(mebibytes=16, **more):
    return pltpu.CompilerParams(vmem_limit_bytes=mebibytes * 2**20, **more)


def any_spec():
    return pl.BlockSpec(memory_space=pl.ANY)


def scalars():
    return pl.BlockSpec(memory_space=pltpu.SMEM)


def packed(place, group_index, frames, arrays):
    width = arrays[0].shape[1]
    quarter = width // 4
    starts, total = [], 0
    for a in arrays:
        starts.append(total)
        total += a.shape[0]

    def kernel(place_ref, group_ref, frames_ref, *refs):
        ins, outs, live_ref = refs[:5], refs[5:9], refs[9]
        first = FRAMES_GROUP * group_ref[0]
        f = frames_ref[...]
        live_ref[...] = jnp.zeros_like(live_ref)
        live_ref[:, 0:128] = jnp.ones((16, 128), F32)
        alive = (f < first) & (f >= first - WINDOW_FRAMES)
        live_ref[:, 0:96] = jnp.broadcast_to(alive.astype(F32), (16, 96))
        spot = place_ref[2] * 2 + place_ref[0]
        for here in range(4):

            @pl.when(spot == here)
            def _():
                for n, q in enumerate((here, here ^ 1, here ^ 2, here ^ 3)):
                    for a, at in zip(ins, starts):
                        outs[n][at : at + a.shape[0], :] = a[:, q * quarter : (q + 1) * quarter]

        for out in outs:
            out[total : total + 16, :] = live_ref[...].astype(BF)

    return pl.pallas_call(
        kernel,
        out_shape=[jax.ShapeDtypeStruct((total + 16, quarter), BF)] * 4,
        in_specs=[scalars(), scalars()] + [pl.BlockSpec()] * 6,
        scratch_shapes=[pltpu.VMEM((16, quarter), F32)],
        compiler_params=room(),
        name="packed",
    )(place, group_index, frames, *[in_hbm(a) for a in arrays])


def attend(sets, queries):
    quarter = 3 * HEAD

    def kernel(*refs):
        set_refs, query_refs, outs = refs[:4], refs[4:8], refs[8:]
        rows = 128
        lane = lax.broadcasted_iota(jnp.int32, (rows, HEAD), 1)
        alive = jnp.concatenate([r[288:304, 0:128] for r in set_refs], axis=1)
        alive = alive.astype(F32)[0:1, :] > 0.5
        stats = [jnp.zeros((rows, HEAD), F32) for _ in range(4)]
        for h in range(3):
            cols = slice(h * HEAD, (h + 1) * HEAD)
            k = jnp.concatenate([r[0:128, cols] for r in set_refs], axis=0)
            v = jnp.concatenate([r[128:256, cols] for r in set_refs], axis=0)
            for r in range(4):
                s = lax.dot_general(
                    query_refs[r][:, cols], k, (((1,), (1,)), ((), ())), preferred_element_type=F32
                ) * (HEAD ** (-0.5))
                s = jnp.where(alive, s, -1e30)
                top = jnp.max(s, axis=1, keepdims=True).astype(BF).astype(F32)
                w = jnp.where(alive, jnp.exp(s - top), 0.0)
                total = jnp.sum(w, axis=1, keepdims=True)
                o = jnp.dot(w.astype(BF), v, preferred_element_type=F32)
                outs[r][:, cols] = o.astype(BF)
                high = total.astype(BF).astype(F32)
                stats[r] = jnp.where(lane == h, top, stats[r])
                stats[r] = jnp.where(lane == 4 + h, high, stats[r])
                stats[r] = jnp.where(lane == 8 + h, total - high, stats[r])
        for r in range(4):
            outs[r][:, quarter:] = stats[r].astype(BF)

    return pl.pallas_call(
        kernel,
        out_shape=[jax.ShapeDtypeStruct((128, 4 * HEAD), BF)] * 4,
        compiler_params=room(),
        name="attend",
    )(*[in_vmem(a) for a in sets], *[in_vmem(a) for a in queries])


def merged(parts):
    def kernel(*refs):
        ins, outs = refs[:4], refs[4:]
        base = 3 * HEAD
        stats = [r[:, base:].astype(F32) for r in ins]
        for h in range(3):
            tops = [s[:, h : h + 1] for s in stats]
            totals = [s[:, 4 + h : 5 + h] + s[:, 8 + h : 9 + h] for s in stats]
            top = jnp.maximum(jnp.maximum(tops[0], tops[1]), jnp.maximum(tops[2], tops[3]))
            scales = [jnp.exp(t - top) for t in tops]
            total = sum(a * b for a, b in zip(scales, totals))
            cols = slice(h * HEAD, (h + 1) * HEAD)
            summed = sum(r[:, cols].astype(F32) * a for r, a in zip(ins, scales))
            mixed = (summed / total).astype(BF)
            for n in range(4):
                outs[n][:, cols] = mixed[32 * n : 32 * n + 32]

    return pl.pallas_call(
        kernel,
        out_shape=[jax.ShapeDtypeStruct((32, 3 * HEAD), BF)] * 4,
        compiler_params=room(),
        name="merged",
    )(*[in_vmem(a) for a in parts])


def streamed(place, timestep, stream, gate_table, mixed, weight):
    width = weight.shape[1]
    quarter = width // 4

    def kernel(place_ref, step_ref, stream_ref, gate_ref, a_ref, b_ref, c_ref, d_ref, w_ref, out_ref):
        spot = place_ref[2] * 2 + place_ref[0]
        for here in range(4):

            @pl.when(spot == here)
            def _():
                total = jnp.zeros(out_ref.shape, F32)
                for ref, q in zip((a_ref, b_ref, c_ref, d_ref), (here, here ^ 2, here ^ 1, here ^ 3)):
                    total = total + jnp.dot(
                        ref[...], w_ref[q * quarter : (q + 1) * quarter, :], preferred_element_type=F32
                    )
                gate = gate_ref[pl.ds(step_ref[0], 1), :]
                out_ref[...] = (stream_ref[...].astype(F32) + gate * total).astype(BF)

    return pl.pallas_call(
        kernel,
        out_shape=jax.ShapeDtypeStruct(stream.shape, BF),
        in_specs=[scalars(), scalars()] + [pl.BlockSpec()] * 7,
        compiler_params=room(),
        name="streamed",
    )(place, timestep, stream, gate_table, *[in_vmem(a) for a in mixed], weight)


def grad_of_input(place, cot, pieces):
    rows, width = cot.shape
    block = 256
    keys = [k for k, _ in pieces]
    count = len(pieces)

    def kernel(place_ref, cot_ref, *refs):
        ins, (out_ref, buf, weight, sem) = refs[:count], refs[count:]
        zl, y, c, zh, x = (place_ref[n] for n in range(5))

        @pl.when(pl.program_id(0) == 0)
        def _():
            copies = []
            for n, (far, step, other) in enumerate(keys):
                zz = 1 - zl if far else zl
                yy = (y + step) % 4
                cc = 1 - c if other else c
                copies.append(
                    pltpu.make_async_copy(ins[n], buf.at[zz * 8 + yy * 2 + cc], sem.at[n])
                )
                copies[-1].start()
            for copy in copies:
                copy.wait()
            for far in range(2):
                for step in range(4):
                    zz = 1 - zh if far else zh
                    xx = (x + 4 - step) % 4
                    at = 12 * (4 * far + step)
                    for t in range(4):
                        part = [buf[t * 4 + k, at : at + 12, :] for k in range(4)]
                        base = pl.multiple_of(zz * 768 + xx * 192 + t * 48, 16)
                        weight[pl.ds(base, 48), :] = jnp.concatenate(part, axis=0)

        out_ref[...] = lax.dot_general(
            cot_ref[...], weight[...], (((1,), (1,)), ((), ())), preferred_element_type=F32
        ).astype(BF)

    return pl.pallas_call(
        kernel,
        grid=(rows // block,),
        out_shape=jax.ShapeDtypeStruct((rows, width), BF),
        in_specs=[scalars(), pl.BlockSpec((block, width), lambda i: (i, 0))] + [any_spec()] * count,
        out_specs=pl.BlockSpec((block, width), lambda i: (i, 0)),
        scratch_shapes=[
            pltpu.VMEM((16, 96, width), BF),
            pltpu.VMEM((width, width), BF),
            pltpu.SemaphoreType.DMA((count,)),
        ],
        compiler_params=room(28, dimension_semantics=("arbitrary",)),
        name="grad_of_input",
    )(place, cot, *[in_vmem(p) for _, p in pieces])


def joined(arrays, first_in_vmem=False):
    rows = [a.shape[0] for a in arrays]

    def kernel(*refs):
        out_ref, at = refs[-1], 0
        for ref, n in zip(refs[:-1], rows):
            out_ref[at : at + n, :] = ref[...]
            at += n

    place_first = in_vmem if first_in_vmem else in_hbm
    return pl.pallas_call(
        kernel,
        out_shape=pltpu.VMEM((sum(rows), arrays[0].shape[1]), arrays[0].dtype),
        compiler_params=room(),
        name="joined",
    )(place_first(arrays[0]), *[in_vmem(a) for a in arrays[1:]])


def weight_pieces(weight):
    on_x = [weight] + [lax.ppermute(weight, "x", turn(k)) for k in (1, 2, 3)]
    on_x = joined(on_x)
    far = lax.ppermute(on_x, "zh", SWAP)
    near = joined([on_x, far], True)
    far = lax.ppermute(near, "zl", SWAP)
    pieces = {(0, 0): near, (1, 0): far}
    for f in range(2):
        pieces[f, 3] = lax.ppermute(pieces[f, 0], "y", turn(1))
        pieces[f, 1] = lax.ppermute(pieces[f, 0], "y", turn(-1))
    pieces[0, 2] = lax.ppermute(pieces[0, 1], "y", turn(-1))
    pieces[1, 2] = lax.ppermute(pieces[1, 3], "y", turn(1))
    out = [((f, step, 0), p) for (f, step), p in pieces.items()]
    out += [((f, step, 1), lax.ppermute(p, "c", SWAP)) for (f, step), p in pieces.items()]
    return out


def own_queries_of(sets):
    def kernel(*refs):
        for n in range(4):
            refs[4][32 * n : 32 * n + 32, :] = refs[n][256:288, :]

    return pl.pallas_call(
        kernel,
        out_shape=jax.ShapeDtypeStruct((128, 3 * HEAD), BF),
        compiler_params=room(),
        name="own_queries",
    )(*[in_vmem(a) for a in sets])


def product_and_split(place, critic_in, critic_cot, got, factor):
    tokens, width = critic_cot.shape
    half = width // 2

    def kernel(place_ref, in_ref, cot_ref, got_ref, send_l, send_r, keep_l, keep_r):
        x = place_ref[4]
        p = pl.program_id(0)
        result = lax.dot_general(
            in_ref[...], cot_ref[...], (((0,), (0,)), ((), ())), preferred_element_type=F32
        ) * factor + got_ref[...].astype(F32)
        for u in range(2):
            chunk = 2 * p + u
            left = result[192 * u : 192 * u + 192, :half]
            right = result[192 * u : 192 * u + 192, half:]
            kept_l = (chunk == x) | (chunk == 3 - x)
            kept_r = (chunk == x) | (chunk == (x ^ 1))

            @pl.when(kept_l)
            def _():
                keep_l[jnp.where(chunk == x, 0, 1)] = left

            @pl.when(jnp.logical_not(kept_l))
            def _():
                send_l[jnp.where(chunk == (x ^ 1), 0, 1)] = left.astype(BF)

            @pl.when(kept_r)
            def _():
                keep_r[jnp.where(chunk == x, 0, 1)] = right

            @pl.when(jnp.logical_not(kept_r))
            def _():
                send_r[jnp.where(chunk == 3 - x, 0, 1)] = right.astype(BF)

    whole = pl.BlockSpec((2, 192, half), lambda p, place: (0, 0, 0))
    return pl.pallas_call(
        kernel,
        grid_spec=pltpu.PrefetchScalarGridSpec(
            num_scalar_prefetch=1,
            grid=(2,),
            in_specs=[
                pl.BlockSpec((tokens, width // 4), lambda p, place: (0, 2 * place[2] + p)),
                pl.BlockSpec((tokens, width), lambda p, place: (0, 0)),
                pl.BlockSpec((width // 4, width), lambda p, place: (p, 0)),
            ],
            out_specs=[whole] * 4,
        ),
        out_shape=[jax.ShapeDtypeStruct((2, 192, half), BF)] * 2
        + [jax.ShapeDtypeStruct((2, 192, half), F32)] * 2,
        compiler_params=room(40, dimension_semantics=("arbitrary",)),
        name="product_and_split",
    )(place, in_hbm(critic_in), critic_cot, in_vmem(got))


def onward_of(keep_l, keep_r, got_l, got_r):
    def kernel(kl, kr, gl, gr, out_l, out_r):
        out_l[...] = (kl[0] + gl[1].astype(F32)).astype(BF)
        out_r[...] = (kr[0] + gr[1].astype(F32)).astype(BF)

    _, rows, cols = keep_l.shape
    block = pl.BlockSpec((1, rows, cols), lambda i: (1, 0, 0))
    return pl.pallas_call(
        kernel,
        grid=(1,),
        in_specs=[block] * 2 + [pl.BlockSpec(memory_space=pltpu.VMEM)] * 2,
        out_specs=[pl.BlockSpec((rows, cols), lambda i: (0, 0))] * 2,
        out_shape=[jax.ShapeDtypeStruct((rows, cols), BF)] * 2,
        compiler_params=room(),
        name="onward",
    )(keep_l, keep_r, in_vmem(got_l), in_vmem(got_r))


def cut_along_y(place, keep_l, keep_r, got_l, got_r, last_l, last_r):
    half = keep_l.shape[2]

    def kernel(place_ref, kl, kr, gl, gr, ll, lr, own, pair, away, total):
        total[:, :half] = kl[0] + gl[0].astype(F32) + ll[...].astype(F32)
        total[:, half:] = kr[0] + gr[0].astype(F32) + lr[...].astype(F32)
        y = place_ref[1]
        for ref, first, yy in ((own, 0, y), (pair, 0, y ^ 1), (away, 0, 3 - y), (away, 2, 3 - (y ^ 1))):
            for z in range(2):
                rows = total[pl.ds(pl.multiple_of(z * 96 + yy * 24, 8), 24), :]
                ref[first + z] = rows.astype(ref.dtype)

    first = pl.BlockSpec((1, 192, half), lambda i: (0, 0, 0))
    sizes = ((2, F32), (2, F32), (4, BF))
    return pl.pallas_call(
        kernel,
        grid=(1,),
        in_specs=[scalars()] + [first] * 2 + [pl.BlockSpec(memory_space=pltpu.VMEM)] * 4,
        out_specs=[pl.BlockSpec((n, 24, 2 * half), lambda i: (0, 0, 0)) for n, _ in sizes],
        out_shape=[jax.ShapeDtypeStruct((n, 24, 2 * half), t) for n, t in sizes],
        scratch_shapes=[pltpu.VMEM((192, 2 * half), F32)],
        compiler_params=room(),
        name="cut_along_y",
    )(place, keep_l, keep_r, *[in_vmem(a) for a in (got_l, got_r, last_l, last_r)])


def for_pair(pair, got):
    def kernel(pair_ref, got_ref, out_ref):
        out_ref[...] = (pair_ref[...] + got_ref[2:4].astype(F32)).astype(BF)

    return pl.pallas_call(
        kernel,
        out_shape=jax.ShapeDtypeStruct(pair.shape, BF),
        compiler_params=room(),
        name="for_pair",
    )(pair, in_vmem(got))


def cut_to_owners(place, own, got, last):
    width = own.shape[2]

    def kernel(place_ref, own_ref, got_ref, last_ref, *outs):
        total = own_ref[...] + got_ref[0:2].astype(F32) + last_ref[...].astype(F32)
        spot = place_ref[0] * 2 + place_ref[3]
        for here in range(4):

            @pl.when(spot == here)
            def _():
                for n in range(4):
                    z, k = (here ^ n) // 2, (here ^ n) % 2
                    outs[n][...] = total[z, 12 * k : 12 * k + 12, :]

    return pl.pallas_call(
        kernel,
        in_specs=[scalars()] + [pl.BlockSpec()] * 3,
        out_shape=[jax.ShapeDtypeStruct((12, width), F32)] * 4,
        compiler_params=room(),
        name="cut_to_owners",
    )(place, own, in_vmem(got), in_vmem(last))


def added(arrays):
    def kernel(*refs):
        refs[-1][...] = (refs[0][...] + refs[1][...]) + (refs[2][...] + refs[3][...])

    return pl.pallas_call(
        kernel,
        out_shape=jax.ShapeDtypeStruct(arrays[0].shape, F32),
        compiler_params=room(),
        name="added",
    )(*[in_vmem(a) for a in arrays])


def weight_gradient(place, critic_in, critic_cot, c, factor):
    half = critic_cot.shape[1] // 2
    theirs = lax.dynamic_slice_in_dim(critic_in, (1 - c) * half, half, 1)
    theirs = (
        lax.dot_general(
            theirs, critic_cot, (((0,), (0,)), ((), ())), preferred_element_type=F32
        )
        * factor
    ).astype(BF)
    got = lax.ppermute(theirs, "c", SWAP)
    send_l, send_r, keep_l, keep_r = product_and_split(place, critic_in, critic_cot, got, factor)
    near = [(0, 1), (1, 0), (2, 3), (3, 2)]
    wrap = [(0, 3), (3, 0), (1, 2), (2, 1)]
    got_l = lax.ppermute(send_l, "x", near)
    got_r = lax.ppermute(send_r, "x", wrap)
    on_l, on_r = onward_of(keep_l, keep_r, got_l, got_r)
    last_l = lax.ppermute(on_l, "x", wrap)
    last_r = lax.ppermute(on_r, "x", near)
    own, pair, away = cut_along_y(place, keep_l, keep_r, got_l, got_r, last_l, last_r)
    got = lax.ppermute(away, "y", wrap)
    last = lax.ppermute(for_pair(pair, got), "y", near)
    cuts = cut_to_owners(place, own, got, last)

    def owner(far_z, far_c):
        spots = [(h, z, k) for h in range(2) for z in range(2) for k in range(2)]
        return [(h * 4 + z * 2 + k, k * 4 + (z ^ far_z) * 2 + (h ^ far_c)) for h, z, k in spots]

    ends = [lax.ppermute(a, ("zh", "zl", "c"), owner(n // 2, n % 2)) for n, a in enumerate(cuts)]
    return added(ends)


def step(
    stream,
    queries,
    new_keys,
    new_values,
    cache_keys,
    cache_values,
    cache_frames,
    group_index,
    timestep,
    gate_table,
    attn_out_weight,
    critic_in,
    critic_cot,
    critic_weight,
):
    zh, x, zl, y, c = (lax.axis_index(a) for a in ("zh", "x", "zl", "y", "c"))
    place = jnp.stack([zl, y, c, zh, x]).astype(jnp.int32)
    near_near, near_far, far_near, far_far = packed(
        place,
        group_index,
        cache_frames,
        (cache_keys[0], new_keys[0], cache_values[0], new_values[0], queries[0]),
    )
    sets = [near_near, lax.ppermute(far_near, "c", SWAP), lax.ppermute(near_far, "zl", SWAP)]
    sets.append(lax.ppermute(lax.ppermute(far_far, "c", SWAP), "zl", SWAP))
    pieces = weight_pieces(critic_weight)

    factor = float(critic_in.shape[0] * 128) ** (-0.5)
    grad_weight = weight_gradient(place, critic_in, critic_cot, c, factor)

    own = own_queries_of(sets)
    all_queries = [own] + [lax.ppermute(own, "y", turn(k)) for k in (1, 2, 3)]
    partial = attend(sets, all_queries)
    parts = [partial[0]] + [lax.ppermute(partial[k], "y", turn(-k)) for k in (1, 2, 3)]
    mixed = merged(parts)
    cross = [(0, 3), (3, 0), (1, 2), (2, 1)]
    mixed = [
        mixed[0],
        lax.ppermute(mixed[1], "c", SWAP),
        lax.ppermute(mixed[2], "zl", SWAP),
        lax.ppermute(mixed[3], ("zl", "c"), cross),
    ]
    stream_out = streamed(place, timestep, stream[0], gate_table, mixed, attn_out_weight)[None]
    grad_in = grad_of_input(place, critic_cot, pieces)
    return (stream_out, grad_in, grad_weight)


def solution(mesh):
    cut = Mesh(mesh.devices.reshape(2, 4, 2, 4, 2), ("zh", "x", "zl", "y", "c"))
    dp, seq = ("zh", "x"), ("zl", "y", "c")
    whole = dp + seq
    return jax.shard_map(
        step,
        mesh=cut,
        in_specs=(
            P(dp, seq, None),
            P(dp, seq, None),
            P(dp, seq, None),
            P(dp, seq, None),
            P(dp, seq, None),
            P(dp, seq, None),
            P(dp, seq),
            P(dp),
            P(dp),
            P(),
            P(),
            P(whole, None),
            P(whole, None),
            P(whole, None),
        ),
        out_specs=(P(dp, seq, None), P(whole, None), P(whole, None)),
        check_vma=False,
    )
```
